256 devices in a mesh: atom: 32 (over x, z_lo, core), chan: 8 (over y, z_hi).
Axes of the slice: x: 4, y: 4, z: 8 (z_hi: 2, z_lo: 4; z = z_hi * 4 + z_lo), core: 2. Of those that a mesh axis runs over, the one named last changes fastest.
Arguments:
- positions: float32 [3, 4096], P(None, 'atom'), may hold values from -9 to 9
- features: bfloat16 [512, 4096], P('chan', 'atom'), may hold values from -6 to 6
- struct_ids: int32 [4096], P('atom'), may hold values from 0 to 31, as said below
- slots: int32 [64, 4096], P(None, 'atom'), may hold values from 0 to 96, as said below
- validity: int32 [64, 4096], P(None, 'atom'), may hold values from 0 to 1, as said below
- radial_in: bfloat16 [512, 128], replicated, may hold values from -72 to 72
- radial_out: bfloat16 [512, 512], P('chan'), may hold values from -0.0234375 to 0.0234375
- mixing: bfloat16 [512, 512], P(None, 'chan'), may hold values from -0.5 to 0.5
- readout: float32 [512], replicated, may hold values from -0.0078125 to 0.0078125
Outputs:
- forces: float32 [3, 4096], P(None, 'atom')
- stress: float32 [9, 32], replicated
The draws below stay inside these ranges and needn't reach their ends.
Inputs may be any that keep to these rules, and one draw needn't show every extreme that they name: `struct_ids`: structure numbers never fall along the atoms and every structure has at least one atom. `slots`: the 64 slot values of one atom are distinct and never equal 48. `validity`: an edge is valid only where its neighbour atom exists and belongs to the same structure.
All inputs are finite; a program needn't handle non-finite values.
Results may differ from the reference program's by a relative error of at most 0.0099.
Values may be sent and summed in bfloat16 or wider, within the bound.
No kernel may reach another device: no remote copies, remote signals or barrier semaphores. Data moves between devices by JAX's collectives and lax.ppermute only.
A program may use at most 64 MiB of HBM per device.

```python
import jax
import jax.numpy as jnp
from jax import lax

C = 512
H = 512
Q = 128
K = 64
RIM = 48
A_DEV = 128
ATOMS = 4096
STRUCTS = 32
N_ATOM = 32


def layout(key):
    cut_key = jax.random.fold_in(key, 11)
    cuts = jax.random.permutation(cut_key, ATOMS - 1)[:STRUCTS - 1] + 1
    atom_index = jnp.arange(ATOMS, dtype=jnp.int32)
    owners = jnp.sum((atom_index[:, None] >= cuts[None, :]).astype(jnp.int32), axis=1).astype(jnp.int32)
    atom_keys = jax.random.split(jax.random.fold_in(key, 12), ATOMS)
    picks = jax.vmap(lambda single: jax.random.permutation(single, 2 * RIM)[:K])(atom_keys)
    slot_values = jnp.where(picks < RIM, picks, picks + 1).T.astype(jnp.int32)
    target = atom_index[None, :] + slot_values - RIM
    inside = (target >= 0) & (target < ATOMS)
    partner = owners[jnp.clip(target, 0, ATOMS - 1)]
    chance = jax.random.randint(jax.random.fold_in(key, 13), (K, ATOMS), 0, 1000)
    limit = 350 + 600 * atom_index // ATOMS
    valid = inside & (partner == owners[None, :]) & (chance < limit[None, :])
    return (owners, slot_values, valid.astype(jnp.int32))


def draw_struct_ids(key, part):
    return layout(key)[0]


def draw_slots(key, part):
    return layout(key)[1]


def draw_validity(key, part):
    return layout(key)[2]


def block_levels(rng, shape, cuts, low, high):
    factor_of = 1.0
    for axis_at, parts in cuts:
        heights = jax.random.uniform(jax.random.fold_in(jax.random.fold_in(rng, 6), axis_at), (parts,), jnp.float32, low / len(cuts), high / len(cuts))
        factor_of = factor_of * jnp.repeat(jnp.exp(heights), shape[axis_at] // parts).reshape((-1,) + (1,) * (len(shape) - 1 - axis_at))
    return factor_of


def scatter_about(own_key, shape, deviation, most, cuts=(), held_as=jnp.bfloat16):
    factor_of = block_levels(own_key, shape, cuts, -0.22, 0.18) if cuts else 1.0
    entries = jax.random.normal(own_key, shape, jnp.float32) * deviation * factor_of
    return jnp.minimum(jnp.maximum(entries, -most), most).astype(held_as)


def setup_inputs(seed: int = 0) -> dict:
    key_of = jax.random.split(jax.random.key(seed), 10)
    return {
        "positions": scatter_about(key_of[0], (3, ATOMS), 1.5, 9.0, ((1, 32),), jnp.float32),
        "features": scatter_about(key_of[1], (C, ATOMS), 1.0, 6.0, ((0, 8), (1, 32))),
        "struct_ids": draw_struct_ids(jax.random.fold_in(key_of[9], 71), 0),
        "slots": draw_slots(jax.random.fold_in(key_of[9], 71), 0),
        "validity": draw_validity(jax.random.fold_in(key_of[9], 71), 0),
        "radial_in": scatter_about(key_of[5], (H, Q), 12.0, 72.0),
        "radial_out": scatter_about(key_of[6], (C, H), (H * 128) ** -0.5, 0.0234375, ((0, 8),)),
        "mixing": scatter_about(key_of[7], (C, C), (C // 4) ** -0.5, 0.5, ((1, 8),)),
        "readout": scatter_about(key_of[8], (C,), (C * K * 16) ** -0.5, 0.0078125, (), jnp.float32),
    }


sharpness = 40.0
reach = 10.0

def dsilu(value):
    sigma = jax.nn.sigmoid(value)
    return sigma * (1.0 + value * (1.0 - sigma))

def radial_terms(vector, radial_in, radial_out):
    dist = jnp.sqrt(1.0 + lax.optimization_barrier(jnp.sum(vector * vector, axis=0)))
    count = radial_in.shape[1]
    centers = jnp.arange(count).astype(jnp.float32) * (reach / count)
    offset = dist[None, :] - centers[:, None]
    bump = jnp.exp(-sharpness * offset * offset)
    basis = bump.astype(jnp.bfloat16)
    slope = (-2.0 * sharpness * offset * bump).astype(jnp.bfloat16)
    pre = jnp.dot(radial_in, basis, preferred_element_type=jnp.float32)
    dpre = jnp.dot(radial_in, slope, preferred_element_type=jnp.float32)
    hidden = jax.nn.silu(pre).astype(jnp.bfloat16)
    dhidden = (dsilu(pre) * dpre).astype(jnp.bfloat16)
    radial = jnp.dot(radial_out, hidden, preferred_element_type=jnp.float32)
    dradial = jnp.dot(radial_out, dhidden, preferred_element_type=jnp.float32)
    return (dist, radial, dradial)

def reference(positions, features, struct_ids, slots, validity, radial_in, radial_out, mixing, readout):
    slot_count = slots.shape[0]

    def block_terms(block):
        start = (block * A_DEV).astype(jnp.int32)
        slot_block = lax.dynamic_slice_in_dim(slots, start, A_DEV, 1)
        valid_block = lax.dynamic_slice_in_dim(validity, start, A_DEV, 1).reshape(-1).astype(jnp.float32)
        atom_index = start + jnp.arange(A_DEV, dtype=jnp.int32)
        partner = jnp.clip(atom_index[None, :] + slot_block - RIM, 0, ATOMS - 1).astype(jnp.int32)
        own_pos = lax.dynamic_slice_in_dim(positions, start, A_DEV, 1)
        vector = (positions[:, partner] - own_pos[:, None, :]).reshape(3, -1)
        far_feat = features[:, partner].reshape(features.shape[0], -1)
        dist, radial, dradial = radial_terms(vector, radial_in, radial_out)
        message = (far_feat * radial).astype(jnp.bfloat16)
        mixed = jnp.dot(mixing, message, preferred_element_type=jnp.float32)
        gmix = (valid_block[None, :] * readout[:, None] * dsilu(mixed)).astype(jnp.bfloat16)
        gmsg = lax.dot_general(mixing, gmix, (((0,), (0,)), ((), ())), preferred_element_type=jnp.float32)
        gdist = lax.optimization_barrier(jnp.sum(gmsg * far_feat.astype(jnp.float32) * dradial, axis=0))
        gvec = gdist * vector / dist
        atomvir = (vector[:, None, :] * gvec[None, :, :]).reshape(9, slot_count, A_DEV).sum(axis=1)
        return (gvec.reshape(3, slot_count, A_DEV), atomvir)
    blocks = jnp.arange(N_ATOM, dtype=jnp.int32)
    gvecs, virs = lax.map(block_terms, blocks)
    gvec_all = jnp.transpose(gvecs, (1, 2, 0, 3)).reshape(3, slot_count, ATOMS)
    atomvir = jnp.transpose(virs, (1, 0, 2)).reshape(9, ATOMS)
    partner_all = jnp.clip(jnp.arange(ATOMS, dtype=jnp.int32)[None, :] + slots - RIM, 0, ATOMS - 1).astype(jnp.int32)
    incoming = jnp.zeros((3, ATOMS), jnp.float32).at[:, partner_all.reshape(-1)].add(-gvec_all.reshape(3, -1))
    forces = gvec_all.sum(axis=1) + incoming
    onehot = (struct_ids[None, :] == jnp.arange(STRUCTS, dtype=jnp.int32)[:, None]).astype(jnp.float32)
    virial = jnp.dot(atomvir, onehot.T, precision=lax.Precision.HIGHEST)
    counts = lax.optimization_barrier(jnp.sum(onehot, axis=1))
    stress = -virial / counts[None, :]
    return (forces, stress)
```

```python
import functools

import jax
import jax.numpy as jnp
from jax import lax
from jax.experimental import pallas as pl
from jax.experimental.pallas import tpu as pltpu
from jax.sharding import Mesh
from jax.sharding import PartitionSpec as P

RIM = 48
LANES = 128
CHUNK = 256
SHARPNESS = 40.0
REACH = 10.0
STRUCTS = 32

VMEM = pl.BlockSpec(memory_space=pltpu.VMEM)
SMEM = pl.BlockSpec(memory_space=pltpu.SMEM)
F32 = jnp.float32
BF16 = jnp.bfloat16


def iota(shape, dim):
    return lax.broadcasted_iota(jnp.int32, shape, dim)


def dot(a, b):
    return jnp.dot(a, b, preferred_element_type=F32)


def dot_t(a, b):
    return lax.dot_general(a, b, (((1,), (1,)), ((), ())), preferred_element_type=F32)


def sigmoid(v):
    return 0.5 + 0.5 * jnp.tanh(0.5 * v)


def pack_kernel(place, feat, rout, mixt, out):
    chans, rows, width = out.shape
    core = place[2]

    @pl.when(core == 0)
    def _():
        for c in range(chans):
            out[c, :, LANES:] = rout[...]

    @pl.when(core != 0)
    def _():
        for c in range(chans):
            out[c, :, LANES:] = mixt[...]

    for c in range(chans):
        out[c, :, :LANES] = feat[...]


def halo_of(core, sib, cross, lane):
    low = jnp.where(core == 0, sib, cross)
    high = jnp.where(core == 0, cross, sib)
    return jnp.where(lane < 64, low, high)


def slot_index(place, slots):
    used = 8
    first = pl.multiple_of(place[3] * used, used)
    rows = slots[pl.ds(first, used), :]
    return (rows + iota(rows.shape, 1) - RIM) & 255


def stage_kernel(place, pos, sib, cross, slots, radial_in, hidden, dhidden, geo):
    core = place[2]
    idx = slot_index(place, slots)
    lane = iota(idx.shape, 1)
    inner = idx & 127
    vecs = []
    for p in range(3):
        own = jnp.broadcast_to(pos[p : p + 1, :], idx.shape)
        ring = halo_of(
            core,
            jnp.broadcast_to(sib[p : p + 1, :], idx.shape),
            jnp.broadcast_to(cross[p : p + 1, :], idx.shape),
            lane,
        )
        far = jnp.where(
            idx < 128,
            jnp.take_along_axis(own, inner, axis=1),
            jnp.take_along_axis(ring, inner, axis=1),
        )
        vecs.append(far - own)
    dist = jnp.sqrt(1.0 + (vecs[0] * vecs[0] + vecs[1] * vecs[1] + vecs[2] * vecs[2]))
    for p in range(3):
        geo[p] = vecs[p]
    geo[3] = dist
    count = radial_in.shape[1]
    centers = iota((count, LANES), 0).astype(F32) * (REACH / count)
    weights = radial_in[...]
    for k in range(8):
        offset = jnp.broadcast_to(dist[k : k + 1, :], (count, LANES)) - centers
        bump = jnp.exp(-SHARPNESS * offset * offset)
        slope = (-2.0 * SHARPNESS * offset * bump).astype(BF16)
        both = jnp.concatenate([bump.astype(BF16), slope], axis=1)
        pre2 = dot(weights, both)
        pre, dpre = pre2[:, :LANES], pre2[:, LANES:]
        sig = sigmoid(pre)
        silu = pre * sig
        at = slice(k * LANES, (k + 1) * LANES)
        hidden[:, at] = silu.astype(BF16)
        dhidden[:, at] = ((sig + silu * (1.0 - sig)) * dpre).astype(BF16)


def main_kernel(
    place, gathered, swapped, cross, hidden, dhidden, geo, slots, valid, ids, readout, out, table_f, w_rad, w_mixt, w_mix, scale
):
    core = place[2]
    channels = table_f.shape[0]

    def keep(ref, w_ref):
        w_ref[...] = ref[:, :, LANES:].reshape(channels, channels)

    @pl.when(core == 0)
    def _():
        keep(gathered, w_rad)
        keep(swapped, w_mixt)

    @pl.when(core != 0)
    def _():
        keep(swapped, w_rad)
        keep(gathered, w_mixt)

    w_mix[...] = w_mixt[...].T
    lane = iota((channels, LANES), 1)
    own_f = gathered[:, :, :LANES].reshape(channels, LANES)
    sib_f = swapped[:, :, :LANES].reshape(channels, LANES)
    cross_f = cross[...].reshape(channels, LANES)
    table_f[:, :LANES] = own_f
    table_f[:, LANES:] = halo_of(core, sib_f, cross_f, lane)
    turned = jnp.concatenate([readout[...]] * 2, axis=0).T
    for j in range(4):
        scale[j * LANES : (j + 1) * LANES, :] = jnp.broadcast_to(turned[:, j : j + 1], (LANES, LANES))

    idx = slot_index(place, slots)
    first = pl.multiple_of(place[3] * 8, 8)
    weight = valid[pl.ds(first, 8), :].astype(F32)
    gdists = []
    onehots = []
    for n in range(1024 // CHUNK):
        per = CHUNK // LANES
        row_of = iota((256, LANES), 0)
        onehot = jnp.concatenate(
            [
                (row_of == jnp.broadcast_to(idx[k : k + 1, :], (256, LANES))).astype(F32).astype(BF16)
                for k in range(n * per, (n + 1) * per)
            ],
            axis=1,
        )
        onehots.append(onehot)
        at = slice(n * CHUNK, (n + 1) * CHUNK)
        far = dot(table_f[...], onehot)
        radial = dot(w_rad[...], hidden[:, at])
        message = (far * radial).astype(BF16)
        mixed = dot(w_mix[...], message)
        sig = sigmoid(mixed)
        slope = sig + mixed * sig * (1.0 - sig)
        wide = jnp.concatenate([scale[...]] * per, axis=1)
        gmix = (wide * slope).astype(BF16)
        gmsg = dot(w_mixt[...], gmix)
        dradial = dot(w_rad[...], dhidden[:, at])
        gdists.append(jnp.sum(gmsg * far * dradial, axis=0, keepdims=True))
    row8 = iota((8, LANES), 0)
    gdist = jnp.zeros((8, LANES), F32)
    for k in range(8):
        per = CHUNK // LANES
        part = gdists[k // per][:, (k % per) * LANES : (k % per + 1) * LANES]
        gdist = jnp.where(row8 == k, jnp.broadcast_to(part, (8, LANES)), gdist)
    over = gdist * weight / geo[3]
    vecs = [geo[p] for p in range(3)]
    gvec = [over * v for v in vecs]

    def total(v):
        return jnp.broadcast_to(jnp.sum(v, axis=0, keepdims=True), (8, LANES))

    zero = jnp.zeros((8, LANES), F32)
    acc = jnp.zeros((8, 256), F32)
    for k in range(8):
        rows = zero
        for p in range(3):
            rows = jnp.where(row8 == p, jnp.broadcast_to(gvec[p][k : k + 1, :], (8, LANES)), rows)
        per = CHUNK // LANES
        hot = onehots[k // per][:, (k % per) * LANES : (k % per + 1) * LANES]
        rest = rows
        for _ in range(3):
            part = rest.astype(BF16)
            acc = acc + dot_t(part, hot)
            rest = rest - part.astype(F32)
    own, ring = -acc[:, :LANES], -acc[:, LANES:]
    for p in range(3):
        own = own + jnp.where(row8 == p, total(gvec[p]), 0.0)
    pairs = ((0, 0), (0, 1), (0, 2), (1, 1), (1, 2), (2, 2))
    vir = jnp.where(row8 == 6, 1.0, zero)
    for j, (p, q) in enumerate(pairs):
        vir = jnp.where(row8 == j, total(vecs[p] * gvec[q]), vir)
    struct = iota((LANES, LANES), 0) & (STRUCTS - 1)
    member = (struct == jnp.broadcast_to(ids[...], (LANES, LANES))).astype(F32).astype(BF16)
    spread = jnp.zeros((8, LANES), F32)
    rest = vir
    for _ in range(3):
        part = rest.astype(BF16)
        spread = spread + dot_t(part, member)
        rest = rest - part.astype(F32)
    lane8 = iota((8, LANES), 1)
    picked = jnp.where((lane8 >> 5) == (row8 & 3), spread, 0.0)
    first_row = total(jnp.where(row8 < 4, picked, 0.0))
    second_row = total(jnp.where(row8 >= 4, picked, 0.0))
    ring = pltpu.roll(ring, 3, 0)
    result = jnp.where(row8 < 3, own, jnp.where(row8 < 6, ring, jnp.where(row8 == 6, first_row, second_row)))
    for c in range(out.shape[0]):
        out[c] = result


def middle_kernel(place, got, out):
    x, zl, core, nx = place[0], place[1], place[2], 4
    row8, lane8 = iota((8, LANES), 0), iota((8, LANES), 1)
    edge = jnp.where(core == 0, jnp.where(zl == 3, -1, 0), jnp.where(zl == 0, 1, 0))
    source = x + edge
    inside = jnp.logical_and(source >= 0, source < nx)
    source = jnp.clip(source, 0, nx - 1)
    whole = got[0]
    for i in range(1, got.shape[0]):
        whole = whole + got[i]

    def over_y(xx, kk):
        v = got[xx * 8 + kk]
        for y in range(1, 4):
            v = v + got[xx * 8 + y * 2 + kk]
        return v

    mine = over_y(x, core)
    near = pltpu.roll(over_y(x, 1 - core), 5, 0)
    far = over_y(source, 1 - core)
    far = jnp.where(inside, far, 0.0)
    low = lane8 < 64
    is_first = core == 0
    near_mask = jnp.logical_xor(low, is_first)
    mine = mine + jnp.where(near_mask, near, 0.0)
    far = jnp.where(near_mask, 0.0, far)
    result = jnp.where(row8 < 3, mine, jnp.where(row8 < 6, far, whole))
    for c in range(out.shape[0]):
        out[c] = result


def final_kernel(place, got, forces, stress):
    zl, core = place[1], place[2]
    whole = got[0]
    for i in range(1, got.shape[0]):
        whole = whole + got[i]
    mine = got[zl * 2] + got[zl * 2 + 1]
    other = (zl + jnp.where(core == 0, 3, 1)) & 3
    ring = got[other * 2] + got[other * 2 + 1]
    forces[...] = mine[:3, :] + ring[3:6, :]
    count = whole[7:8, 64:96] * 0.125
    where_is = {(0, 0): 0, (0, 1): 1, (0, 2): 2, (1, 1): 3, (1, 2): 4, (2, 2): 5}
    for p in range(3):
        for q in range(3):
            j = where_is[(min(p, q), max(p, q))]
            value = whole[6 + j // 4 : 7 + j // 4, (j % 4) * 32 : (j % 4) * 32 + 32]
            stress[3 * p + q : 3 * p + q + 1, :] = -value / count


def local(positions, features, struct_ids, slots, validity, radial_in, radial_out, mixing, readout):
    place = jnp.stack(
        [
            lax.axis_index("x"),
            lax.axis_index("zl"),
            lax.axis_index("k"),
            lax.axis_index(("y", "zh")),
        ]
    ).astype(jnp.int32)
    atoms = ("x", "zl", "k")
    domains = lax.axis_size(atoms)
    siblings = [(d, d ^ 1) for d in range(domains)]
    crossing = [(d, d + 1) for d in range(1, domains - 1, 2)]
    crossing = crossing + [(j, i) for i, j in crossing]
    channels = readout.shape[0]
    packed = pl.pallas_call(
        pack_kernel,
        out_shape=jax.ShapeDtypeStruct((8, features.shape[0], LANES + channels), BF16),
        in_specs=[SMEM, VMEM, VMEM, VMEM],
        out_specs=VMEM,
        name="pack",
    )(place, features, radial_out, mixing.T)
    gathered = lax.all_to_all(packed, ("y", "zh"), 0, 0, tiled=True)
    pos_sib = lax.ppermute(positions, atoms, siblings)
    pos_cross = lax.ppermute(positions, atoms, crossing)
    edges = 8 * LANES
    hidden, dhidden, geo = pl.pallas_call(
        stage_kernel,
        out_shape=(
            jax.ShapeDtypeStruct((channels, edges), BF16),
            jax.ShapeDtypeStruct((channels, edges), BF16),
            jax.ShapeDtypeStruct((4, 8, LANES), F32),
        ),
        in_specs=[SMEM] + [VMEM] * 5,
        out_specs=(VMEM, VMEM, VMEM),
        cost_estimate=pl.CostEstimate(flops=5_000_000_000, bytes_accessed=4_000_000, transcendentals=1_000_000),
        name="stage",
    )(place, positions, pos_sib, pos_cross, slots, radial_in)
    swapped = lax.ppermute(gathered, atoms, siblings)
    cross = lax.ppermute(gathered[:, :, :LANES], atoms, crossing)
    message = pl.pallas_call(
        main_kernel,
        out_shape=jax.ShapeDtypeStruct((32, 8, LANES), F32),
        in_specs=[SMEM] + [VMEM] * 10,
        out_specs=VMEM,
        scratch_shapes=[
            pltpu.VMEM((channels, 2 * LANES), BF16),
            pltpu.VMEM((channels, channels), BF16),
            pltpu.VMEM((channels, channels), BF16),
            pltpu.VMEM((channels, channels), BF16),
            pltpu.VMEM((channels, LANES), F32),
        ],
        name="main",
    )(
        place,
        gathered,
        swapped,
        cross,
        hidden,
        dhidden,
        geo,
        slots,
        validity,
        struct_ids.reshape(1, LANES),
        readout.reshape(4, LANES),
    )
    got = lax.all_to_all(message, ("x", "y", "k"), 0, 0, tiled=True)
    message = pl.pallas_call(
        middle_kernel,
        out_shape=jax.ShapeDtypeStruct((8, 8, LANES), F32),
        in_specs=[SMEM, VMEM],
        out_specs=VMEM,
        name="middle",
    )(place, got)
    got = lax.all_to_all(message, ("zl", "zh"), 0, 0, tiled=True)
    return pl.pallas_call(
        final_kernel,
        out_shape=(
            jax.ShapeDtypeStruct((3, LANES), F32),
            jax.ShapeDtypeStruct((9, STRUCTS), F32),
        ),
        in_specs=[SMEM, VMEM],
        out_specs=(VMEM, VMEM),
        name="final",
    )(place, got)


def solution(mesh):
    fine = Mesh(mesh.devices.reshape(4, 4, 2, 4, 2), ("x", "zl", "k", "y", "zh"))
    atoms, chans = ("x", "zl", "k"), ("y", "zh")
    placed = (
        P(None, atoms),
        P(chans, atoms),
        P(atoms),
        P(None, atoms),
        P(None, atoms),
        P(),
        P(chans, None),
        P(None, chans),
        P(),
    )
    return jax.shard_map(
        local, mesh=fine, in_specs=placed, out_specs=(P(None, atoms), P()), check_vma=False
    )
```

```python
import jax
import jax.numpy as jnp
from jax import lax
from jax.experimental import pallas as pl
from jax.experimental.pallas import tpu as pltpu
from jax.sharding import Mesh
from jax.sharding import PartitionSpec as P


RIM = 48
LANES = 128
CHUNK = 256
SHARPNESS = 40.0
REACH = 10.0
STRUCTS = 32

VMEM = pl.BlockSpec(memory_space=pltpu.VMEM)
F32 = jnp.float32
BF16 = jnp.bfloat16


def kernel(body, outs, mib, scratch=(), cost=1, space=pltpu.VMEM):
    def call(*args):
        return pl.pallas_call(
            body,
            out_shape=[jax.ShapeDtypeStruct(shape, dtype) for shape, dtype in outs],
            in_specs=[pl.BlockSpec(memory_space=space)] * len(args),
            out_specs=[VMEM] * len(outs),
            scratch_shapes=list(scratch),
            compiler_params=pltpu.CompilerParams(vmem_limit_bytes=mib << 20),
            cost_estimate=pl.CostEstimate(flops=cost * 1_000_000_000, bytes_accessed=100_000, transcendentals=0),
        )(*args)

    return call


def iota(shape, dim):
    return lax.broadcasted_iota(jnp.int32, shape, dim)


def dot(a, b):
    return jnp.dot(a, b, preferred_element_type=F32)


def dot_t(a, b):
    return lax.dot_general(a, b, (((1,), (1,)), ((), ())), preferred_element_type=F32)


def sigmoid(v):
    return 0.5 + 0.5 * jnp.tanh(0.5 * v)


def where_am_i():
    return lax.axis_index("x"), lax.axis_index("zl"), lax.axis_index("k")


def slot_group():
    return lax.axis_index("y") * 2 + lax.axis_index("zh")


def pack_kernel(feat, weights, feat_z, weights_z, out):
    rows = feat.shape[0]
    zh = lax.axis_index("zh")
    here, there = pl.multiple_of(zh * rows, rows), pl.multiple_of((1 - zh) * rows, rows)
    for c in range(out.shape[0]):
        out[c, pl.ds(here, rows), :LANES] = feat[...]
        out[c, pl.ds(here, rows), LANES:] = weights[...]
        out[c, pl.ds(there, rows), :LANES] = feat_z[...]
        out[c, pl.ds(there, rows), LANES:] = weights_z[...]


def halo_of(core, sib, cross, lane):
    low = jnp.where(core == 0, sib, cross)
    high = jnp.where(core == 0, cross, sib)
    return jnp.where(lane < 64, low, high)


def own_rows(ref):
    used = 8
    first = pl.multiple_of(slot_group() * used, used)
    return ref[pl.ds(first, used), :]


def slot_index(slots):
    rows = own_rows(slots)
    return (rows + iota(rows.shape, 1) - RIM) & 255


def stage_kernel(pos, sib, cross, slots, radial_in, hidden, dhidden, geo):
    core = lax.axis_index("k")
    idx = slot_index(slots)
    lane = iota(idx.shape, 1)
    inner = idx & 127
    vecs = []
    for p in range(3):
        own = jnp.broadcast_to(pos[p : p + 1, :], idx.shape)
        ring = halo_of(
            core,
            jnp.broadcast_to(sib[p : p + 1, :], idx.shape),
            jnp.broadcast_to(cross[p : p + 1, :], idx.shape),
            lane,
        )
        far = jnp.where(
            idx < 128,
            jnp.take_along_axis(own, inner, axis=1),
            jnp.take_along_axis(ring, inner, axis=1),
        )
        vecs.append(far - own)
    dist = jnp.sqrt(1.0 + (vecs[0] * vecs[0] + vecs[1] * vecs[1] + vecs[2] * vecs[2]))
    for p in range(3):
        geo[p] = vecs[p]
    geo[3] = dist
    count = radial_in.shape[1]
    centers = iota((count, LANES), 0).astype(F32) * (REACH / count)
    weights = radial_in[...]
    for k in range(8):
        offset = jnp.broadcast_to(dist[k : k + 1, :], (count, LANES)) - centers
        bump = jnp.exp(-SHARPNESS * offset * offset)
        slope = (-2.0 * SHARPNESS * offset * bump).astype(BF16)
        both = jnp.concatenate([bump.astype(BF16), slope], axis=1)
        pre2 = dot(weights, both)
        pre, dpre = pre2[:, :LANES], pre2[:, LANES:]
        sig = sigmoid(pre)
        silu = pre * sig
        at = slice(k * LANES, (k + 1) * LANES)
        hidden[:, at] = silu.astype(BF16)
        dhidden[:, at] = ((sig + silu * (1.0 - sig)) * dpre).astype(BF16)


def radial_kernel(gathered, swapped, hidden, dhidden, radial, dradial, mix, mixt):
    core = lax.axis_index("k")
    channels = mix.shape[0]

    def run(w_rad, w_mixt):
        weights = w_rad[:, :, LANES:].reshape(channels, channels)
        for n in range(hidden.shape[1] // CHUNK):
            at = slice(n * CHUNK, (n + 1) * CHUNK)
            radial[:, at] = dot(weights, hidden[:, at])
            dradial[:, at] = dot(weights, dhidden[:, at])
        turned = w_mixt[:, :, LANES:].reshape(channels, channels)
        mixt[...] = turned
        mix[...] = turned.T

    @pl.when(core == 0)
    def _():
        run(gathered, swapped)

    @pl.when(core != 0)
    def _():
        run(swapped, gathered)


def main_kernel(
    own, sib, cross, radial, dradial, mix, mixt, geo, slots, valid, ids, readout, out, table_f, scale
):
    core = lax.axis_index("k")
    channels = table_f.shape[0]
    lane = iota((channels, LANES), 1)
    own_f = own[:, :, :LANES].reshape(channels, LANES)
    sib_f = sib[:, :, :LANES].reshape(channels, LANES)
    cross_f = cross[...].reshape(channels, LANES)
    table_f[:, :LANES] = own_f
    table_f[:, LANES:] = halo_of(core, sib_f, cross_f, lane)
    turned = jnp.concatenate([readout[...]] * 2, axis=0).T
    for j in range(4):
        scale[j * LANES : (j + 1) * LANES, :] = jnp.broadcast_to(turned[:, j : j + 1], (LANES, LANES))

    idx = slot_index(slots)
    weight = own_rows(valid).astype(F32)
    gdists = []
    onehots = []
    for n in range(1024 // CHUNK):
        per = CHUNK // LANES
        row_of = iota((256, LANES), 0)
        onehot = jnp.concatenate(
            [
                (row_of == jnp.broadcast_to(idx[k : k + 1, :], (256, LANES))).astype(F32).astype(BF16)
                for k in range(n * per, (n + 1) * per)
            ],
            axis=1,
        )
        onehots.append(onehot)
        at = slice(n * CHUNK, (n + 1) * CHUNK)
        far = dot(table_f[...], onehot)
        message = (far * radial[:, at]).astype(BF16)
        mixed = dot(mix[...], message)
        sig = sigmoid(mixed)
        slope = sig + mixed * sig * (1.0 - sig)
        wide = jnp.concatenate([scale[...]] * per, axis=1)
        gmix = (wide * slope).astype(BF16)
        gmsg = dot(mixt[...], gmix)
        gdists.append(jnp.sum(gmsg * far * dradial[:, at], axis=0, keepdims=True))
    row8 = iota((8, LANES), 0)
    gdist = jnp.zeros((8, LANES), F32)
    for k in range(8):
        per = CHUNK // LANES
        part = gdists[k // per][:, (k % per) * LANES : (k % per + 1) * LANES]
        gdist = jnp.where(row8 == k, jnp.broadcast_to(part, (8, LANES)), gdist)
    over = gdist * weight / geo[3]
    vecs = [geo[p] for p in range(3)]
    gvec = [over * v for v in vecs]

    def total(v):
        return jnp.broadcast_to(jnp.sum(v, axis=0, keepdims=True), (8, LANES))

    zero = jnp.zeros((8, LANES), F32)
    acc = jnp.zeros((8, 256), F32)
    for k in range(8):
        rows = zero
        for p in range(3):
            rows = jnp.where(row8 == p, jnp.broadcast_to(gvec[p][k : k + 1, :], (8, LANES)), rows)
        per = CHUNK // LANES
        hot = onehots[k // per][:, (k % per) * LANES : (k % per + 1) * LANES]
        rest = rows
        for _ in range(3):
            part = rest.astype(BF16)
            acc = acc + dot_t(part, hot)
            rest = rest - part.astype(F32)
    mine, ring = -acc[:, :LANES], -acc[:, LANES:]
    for p in range(3):
        mine = mine + jnp.where(row8 == p, total(gvec[p]), 0.0)
    pairs = ((0, 0), (0, 1), (0, 2), (1, 1), (1, 2), (2, 2))
    vir = jnp.where(row8 == 6, 1.0, zero)
    for j, (p, q) in enumerate(pairs):
        vir = jnp.where(row8 == j, total(vecs[p] * gvec[q]), vir)
    struct = iota((LANES, LANES), 0) & (STRUCTS - 1)
    member = (struct == jnp.broadcast_to(ids[...], (LANES, LANES))).astype(F32).astype(BF16)
    spread = jnp.zeros((8, LANES), F32)
    rest = vir
    for _ in range(3):
        part = rest.astype(BF16)
        spread = spread + dot_t(part, member)
        rest = rest - part.astype(F32)
    lane8 = iota((8, LANES), 1)
    picked = jnp.where((lane8 >> 5) == (row8 & 3), spread, 0.0)
    first_row = total(jnp.where(row8 < 4, picked, 0.0))
    second_row = total(jnp.where(row8 >= 4, picked, 0.0))
    ring = pltpu.roll(ring, 3, 0)
    result = jnp.where(row8 < 3, mine, jnp.where(row8 < 6, ring, jnp.where(row8 == 6, first_row, second_row)))
    for c in range(out.shape[0]):
        out[c] = result


def middle_kernel(got, out):
    (x, zl, core), nx = where_am_i(), 4
    row8, lane8 = iota((8, LANES), 0), iota((8, LANES), 1)
    edge = jnp.where(core == 0, jnp.where(zl == 3, -1, 0), jnp.where(zl == 0, 1, 0))
    source = x + edge
    inside = jnp.logical_and(source >= 0, source < nx)
    source = jnp.clip(source, 0, nx - 1)
    whole = got[0]
    for i in range(1, got.shape[0]):
        whole = whole + got[i]

    def over_y(xx, kk):
        v = got[xx * 8 + kk]
        for y in range(1, 4):
            v = v + got[xx * 8 + y * 2 + kk]
        return v

    mine = over_y(x, core)
    near = pltpu.roll(over_y(x, 1 - core), 5, 0)
    far = over_y(source, 1 - core)
    far = jnp.where(inside, far, 0.0)
    low = lane8 < 64
    is_first = core == 0
    near_mask = jnp.logical_xor(low, is_first)
    mine = mine + jnp.where(near_mask, near, 0.0)
    far = jnp.where(near_mask, 0.0, far)
    result = jnp.where(row8 < 3, mine, jnp.where(row8 < 6, far, whole))
    for c in range(out.shape[0]):
        out[c] = result


def final_kernel(got, forces, stress):
    _, zl, core = where_am_i()
    whole = got[0]
    for i in range(1, got.shape[0]):
        whole = whole + got[i]
    mine = got[zl * 2] + got[zl * 2 + 1]
    other = (zl + jnp.where(core == 0, 3, 1)) & 3
    ring = got[other * 2] + got[other * 2 + 1]
    forces[...] = mine[:3, :] + ring[3:6, :]
    count = whole[7:8, 64:96] * 0.125
    where_is = {(0, 0): 0, (0, 1): 1, (0, 2): 2, (1, 1): 3, (1, 2): 4, (2, 2): 5}
    for p in range(3):
        for q in range(3):
            j = where_is[(min(p, q), max(p, q))]
            value = whole[6 + j // 4 : 7 + j // 4, (j % 4) * 32 : (j % 4) * 32 + 32]
            stress[3 * p + q : 3 * p + q + 1, :] = -value / count


def chip_to_chip():
    pairs = []
    for x in range(4):
        for zl in range(4):
            if x == 3 and zl == 3:
                continue
            for y in range(4):
                for zh in range(2):
                    here = (((x * 4 + zl) * 2 + 1) * 4 + y) * 2 + zh
                    if zl < 3:
                        there = (((x * 4 + zl + 1) * 2) * 4 + y) * 2 + zh
                    else:
                        there = ((((x + 1) * 4) * 2) * 4 + y) * 2 + (1 - zh)
                    pairs += [(here, there), (there, here)]
    return pairs


def z_partners(mirrored):
    pairs = []
    for x in range(4):
        for zl in range(4):
            for core in range(2):
                for y in range(4):
                    for zh in range(2):
                        other = 3 - zl if mirrored else zl
                        here = (((x * 4 + zl) * 2 + core) * 4 + y) * 2 + zh
                        there = (((x * 4 + other) * 2 + core) * 4 + y) * 2 + (1 - zh)
                        pairs.append((here, there))
    return pairs


def local(positions, features, struct_ids, slots, validity, radial_in, radial_out, mixing, readout):
    atoms = ("x", "zl", "k")
    domains = lax.axis_size(atoms)
    siblings = [(d, d ^ 1) for d in range(domains)]
    crossing = chip_to_chip()
    everyone = ("x", "zl", "k", "y", "zh")
    channels, edges = readout.shape[0], 8 * LANES
    rows = features.shape[0]
    feat_z = lax.ppermute(features, everyone, z_partners(False))
    weights = jnp.where(lax.axis_index("k") == 0, radial_out, mixing.T)
    weights_z = lax.ppermute(weights, everyone, z_partners(True))
    packed = kernel(pack_kernel, [((4, 2 * rows, LANES + channels), BF16)], 4)(
        features, weights, feat_z, weights_z
    )[0]
    gathered = lax.all_to_all(packed, "y", 0, 0, tiled=True)
    pos_sib = lax.ppermute(positions, atoms, siblings)
    pos_cross = lax.ppermute(positions, everyone, crossing)
    hidden, dhidden, geo = kernel(
        stage_kernel,
        [((channels, edges), BF16), ((channels, edges), BF16), ((4, 8, LANES), F32)],
        16,
        cost=3,
    )(positions, pos_sib, pos_cross, slots, radial_in)
    cross = lax.ppermute(gathered[:, :, :LANES], everyone, crossing)
    swapped = lax.ppermute(gathered, atoms, siblings)
    radial, dradial, mix, mixt = kernel(
        radial_kernel,
        [((channels, edges), F32)] * 2 + [((channels, channels), BF16)] * 2,
        12,
        cost=2,
    )(gathered, swapped, hidden, dhidden)
    message = kernel(
        main_kernel,
        [((32, 8, LANES), F32)],
        20,
        scratch=[pltpu.VMEM((channels, 2 * LANES), BF16), pltpu.VMEM((channels, LANES), F32)],
        cost=4,
    )(
        gathered,
        swapped,
        cross,
        radial,
        dradial,
        mix,
        mixt,
        geo,
        slots,
        validity,
        struct_ids.reshape(1, LANES),
        readout.reshape(4, LANES),
    )[0]
    got = lax.all_to_all(message, ("x", "y", "k"), 0, 0, tiled=True)
    message = kernel(middle_kernel, [((8, 8, LANES), F32)], 4)(got)[0]
    got = lax.all_to_all(message, ("zl", "zh"), 0, 0, tiled=True)
    return tuple(kernel(final_kernel, [((3, LANES), F32), ((9, STRUCTS), F32)], 4)(got))


def solution(mesh):
    fine = Mesh(mesh.devices.reshape(4, 4, 2, 4, 2), ("x", "zl", "k", "y", "zh"))
    atoms, chans = ("x", "zl", "k"), ("y", "zh")
    placed = (
        P(None, atoms),
        P(chans, atoms),
        P(atoms),
        P(None, atoms),
        P(None, atoms),
        P(),
        P(chans, None),
        P(None, chans),
        P(),
    )
    return jax.shard_map(
        local, mesh=fine, in_specs=placed, out_specs=(P(None, atoms), P()), check_vma=False
    )
```

```python
import jax
import jax.numpy as jnp
from jax import lax
from jax.experimental import pallas as pl
from jax.experimental.pallas import tpu as pltpu
from jax.sharding import Mesh
from jax.sharding import PartitionSpec as P


RIM = 48
LANES = 128
CHUNK = 256
SHARPNESS = 40.0
REACH = 10.0
STRUCTS = 32

VMEM = pl.BlockSpec(memory_space=pltpu.VMEM)
F32 = jnp.float32
BF16 = jnp.bfloat16


def kernel(body, outs, mib, scratch=(), cost=1, space=pltpu.VMEM):
    def call(*args):
        return pl.pallas_call(
            body,
            out_shape=[jax.ShapeDtypeStruct(shape, dtype) for shape, dtype in outs],
            in_specs=[pl.BlockSpec(memory_space=space)] * len(args),
            out_specs=[VMEM] * len(outs),
            scratch_shapes=list(scratch),
            compiler_params=pltpu.CompilerParams(vmem_limit_bytes=mib << 20),
            cost_estimate=pl.CostEstimate(flops=cost * 1_000_000_000, bytes_accessed=100_000, transcendentals=0),
        )(*args)

    return call


def iota(shape, dim):
    return lax.broadcasted_iota(jnp.int32, shape, dim)


def dot(a, b):
    return jnp.dot(a, b, preferred_element_type=F32)


def dot_t(a, b):
    return lax.dot_general(a, b, (((1,), (1,)), ((), ())), preferred_element_type=F32)


def sigmoid(v):
    return 0.5 + 0.5 * jnp.tanh(0.5 * v)


def where_am_i():
    return lax.axis_index("x"), lax.axis_index("zl"), lax.axis_index("k")


def slot_group():
    return lax.axis_index("y") * 2 + lax.axis_index("zh")


def pack_kernel(here_shard, there_shard, out):
    rows = here_shard.shape[0]
    zh = lax.axis_index("zh")
    here, there = pl.multiple_of(zh * rows, rows), pl.multiple_of((1 - zh) * rows, rows)
    for c in range(out.shape[0]):
        out[c, pl.ds(here, rows), :] = here_shard[...]
        out[c, pl.ds(there, rows), :] = there_shard[...]


def halo_of(core, sib, cross, lane):
    low = jnp.where(core == 0, sib, cross)
    high = jnp.where(core == 0, cross, sib)
    return jnp.where(lane < 64, low, high)


def own_rows(ref):
    used = 8
    first = pl.multiple_of(slot_group() * used, used)
    return ref[pl.ds(first, used), :]


def slot_index(slots):
    rows = own_rows(slots)
    return (rows + iota(rows.shape, 1) - RIM) & 255


def stage_kernel(pos, sib, cross, slots, radial_in, hidden, dhidden, geo):
    core = lax.axis_index("k")
    idx = slot_index(slots)
    lane = iota(idx.shape, 1)
    inner = idx & 127
    vecs = []
    for p in range(3):
        own = jnp.broadcast_to(pos[p : p + 1, :], idx.shape)
        ring = halo_of(
            core,
            jnp.broadcast_to(sib[p : p + 1, :], idx.shape),
            jnp.broadcast_to(cross[p : p + 1, :], idx.shape),
            lane,
        )
        far = jnp.where(
            idx < 128,
            jnp.take_along_axis(own, inner, axis=1),
            jnp.take_along_axis(ring, inner, axis=1),
        )
        vecs.append(far - own)
    dist = jnp.sqrt(1.0 + (vecs[0] * vecs[0] + vecs[1] * vecs[1] + vecs[2] * vecs[2]))
    for p in range(3):
        geo[p] = vecs[p]
    geo[3] = dist
    count = radial_in.shape[1]
    centers = iota((count, LANES), 0).astype(F32) * (REACH / count)
    weights = radial_in[...]
    for k in range(8):
        offset = jnp.broadcast_to(dist[k : k + 1, :], (count, LANES)) - centers
        bump = jnp.exp(-SHARPNESS * offset * offset)
        slope = (-2.0 * SHARPNESS * offset * bump).astype(BF16)
        both = jnp.concatenate([bump.astype(BF16), slope], axis=1)
        pre2 = dot(weights, both)
        pre, dpre = pre2[:, :LANES], pre2[:, LANES:]
        sig = sigmoid(pre)
        silu = pre * sig
        at = slice(k * LANES, (k + 1) * LANES)
        hidden[:, at] = silu.astype(BF16)
        dhidden[:, at] = ((sig + silu * (1.0 - sig)) * dpre).astype(BF16)


def radial_kernel(gathered, swapped, hidden, dhidden, radial, dradial, mix, mixt):
    core = lax.axis_index("k")
    channels = mix.shape[0]

    def run(w_rad, w_mixt):
        weights = w_rad[:, :, LANES:].reshape(channels, channels)
        for n in range(hidden.shape[1] // CHUNK):
            at = slice(n * CHUNK, (n + 1) * CHUNK)
            radial[:, at] = dot(weights, hidden[:, at])
            dradial[:, at] = dot(weights, dhidden[:, at])
        turned = w_mixt[:, :, LANES:].reshape(channels, channels)
        mixt[...] = turned
        mix[...] = turned.T

    @pl.when(core == 0)
    def _():
        run(gathered, swapped)

    @pl.when(core != 0)
    def _():
        run(swapped, gathered)


def main_kernel(
    own, sib, cross, radial, dradial, mix, mixt, geo, slots, valid, ids, readout, out, table_f, scale
):
    core = lax.axis_index("k")
    channels = table_f.shape[0]
    lane = iota((channels, LANES), 1)
    own_f = own[:, :, :LANES].reshape(channels, LANES)
    sib_f = sib[:, :, :LANES].reshape(channels, LANES)
    cross_f = cross[...].reshape(channels, LANES)
    table_f[:, :LANES] = own_f
    table_f[:, LANES:] = halo_of(core, sib_f, cross_f, lane)
    turned = jnp.concatenate([readout[...]] * 2, axis=0).T
    for j in range(4):
        scale[j * LANES : (j + 1) * LANES, :] = jnp.broadcast_to(turned[:, j : j + 1], (LANES, LANES))

    idx = slot_index(slots)
    weight = own_rows(valid).astype(F32)
    gdists = []
    onehots = []
    for n in range(1024 // CHUNK):
        per = CHUNK // LANES
        row_of = iota((256, LANES), 0)
        onehot = jnp.concatenate(
            [
                (row_of == jnp.broadcast_to(idx[k : k + 1, :], (256, LANES))).astype(F32).astype(BF16)
                for k in range(n * per, (n + 1) * per)
            ],
            axis=1,
        )
        onehots.append(onehot)
        at = slice(n * CHUNK, (n + 1) * CHUNK)
        far = dot(table_f[...], onehot)
        message = (far * radial[:, at]).astype(BF16)
        mixed = dot(mix[...], message)
        sig = sigmoid(mixed)
        slope = sig + mixed * sig * (1.0 - sig)
        wide = jnp.concatenate([scale[...]] * per, axis=1)
        gmix = (wide * slope).astype(BF16)
        gmsg = dot(mixt[...], gmix)
        gdists.append(jnp.sum(gmsg * far * dradial[:, at], axis=0, keepdims=True))
    row8 = iota((8, LANES), 0)
    gdist = jnp.zeros((8, LANES), F32)
    for k in range(8):
        per = CHUNK // LANES
        part = gdists[k // per][:, (k % per) * LANES : (k % per + 1) * LANES]
        gdist = jnp.where(row8 == k, jnp.broadcast_to(part, (8, LANES)), gdist)
    over = gdist * weight / geo[3]
    vecs = [geo[p] for p in range(3)]
    gvec = [over * v for v in vecs]

    def total(v):
        return jnp.broadcast_to(jnp.sum(v, axis=0, keepdims=True), (8, LANES))

    zero = jnp.zeros((8, LANES), F32)
    acc = jnp.zeros((8, 256), F32)
    for k in range(8):
        rows = zero
        for p in range(3):
            rows = jnp.where(row8 == p, jnp.broadcast_to(gvec[p][k : k + 1, :], (8, LANES)), rows)
        per = CHUNK // LANES
        hot = onehots[k // per][:, (k % per) * LANES : (k % per + 1) * LANES]
        rest = rows
        for _ in range(3):
            part = rest.astype(BF16)
            acc = acc + dot_t(part, hot)
            rest = rest - part.astype(F32)
    mine, ring = -acc[:, :LANES], -acc[:, LANES:]
    for p in range(3):
        mine = mine + jnp.where(row8 == p, total(gvec[p]), 0.0)
    pairs = ((0, 0), (0, 1), (0, 2), (1, 1), (1, 2), (2, 2))
    vir = jnp.where(row8 == 6, 1.0, zero)
    for j, (p, q) in enumerate(pairs):
        vir = jnp.where(row8 == j, total(vecs[p] * gvec[q]), vir)
    struct = iota((LANES, LANES), 0) & (STRUCTS - 1)
    member = (struct == jnp.broadcast_to(ids[...], (LANES, LANES))).astype(F32).astype(BF16)
    spread = jnp.zeros((8, LANES), F32)
    rest = vir
    for _ in range(3):
        part = rest.astype(BF16)
        spread = spread + dot_t(part, member)
        rest = rest - part.astype(F32)
    lane8 = iota((8, LANES), 1)
    picked = jnp.where((lane8 >> 5) == (row8 & 3), spread, 0.0)
    first_row = total(jnp.where(row8 < 4, picked, 0.0))
    second_row = total(jnp.where(row8 >= 4, picked, 0.0))
    ring = pltpu.roll(ring, 3, 0)
    result = jnp.where(row8 < 3, mine, jnp.where(row8 < 6, ring, jnp.where(row8 == 6, first_row, second_row)))
    for c in range(out.shape[0]):
        out[c] = result


def middle_kernel(got, out):
    (x, zl, core), nx = where_am_i(), 4
    row8, lane8 = iota((8, LANES), 0), iota((8, LANES), 1)
    edge = jnp.where(core == 0, jnp.where(zl == 3, -1, 0), jnp.where(zl == 0, 1, 0))
    source = x + edge
    inside = jnp.logical_and(source >= 0, source < nx)
    source = jnp.clip(source, 0, nx - 1)
    whole = got[0]
    for i in range(1, got.shape[0]):
        whole = whole + got[i]

    def over_y(xx, kk):
        v = got[xx * 8 + kk]
        for y in range(1, 4):
            v = v + got[xx * 8 + y * 2 + kk]
        return v

    mine = over_y(x, core)
    near = pltpu.roll(over_y(x, 1 - core), 5, 0)
    far = over_y(source, 1 - core)
    far = jnp.where(inside, far, 0.0)
    low = lane8 < 64
    is_first = core == 0
    near_mask = jnp.logical_xor(low, is_first)
    mine = mine + jnp.where(near_mask, near, 0.0)
    far = jnp.where(near_mask, 0.0, far)
    result = jnp.where(row8 < 3, mine, jnp.where(row8 < 6, far, whole))
    for c in range(out.shape[0]):
        out[c] = result


def final_kernel(got, forces, stress):
    _, zl, core = where_am_i()
    whole = got[0]
    for i in range(1, got.shape[0]):
        whole = whole + got[i]
    mine = got[zl * 2] + got[zl * 2 + 1]
    other = (zl + jnp.where(core == 0, 3, 1)) & 3
    ring = got[other * 2] + got[other * 2 + 1]
    forces[...] = mine[:3, :] + ring[3:6, :]
    count = whole[7:8, 64:96] * 0.125
    where_is = {(0, 0): 0, (0, 1): 1, (0, 2): 2, (1, 1): 3, (1, 2): 4, (2, 2): 5}
    for p in range(3):
        for q in range(3):
            j = where_is[(min(p, q), max(p, q))]
            value = whole[6 + j // 4 : 7 + j // 4, (j % 4) * 32 : (j % 4) * 32 + 32]
            stress[3 * p + q : 3 * p + q + 1, :] = -value / count


def chip_to_chip():
    pairs = []
    for x in range(4):
        for zl in range(4):
            for y in range(4):
                for zh in range(2):
                    here = (((x * 4 + zl) * 2 + 1) * 4 + y) * 2 + zh
                    x2, zl2, zh2 = (x + (zl == 3)) % 4, (zl + 1) % 4, zh ^ (zl == 3)
                    there = ((x2 * 4 + zl2) * 2 * 4 + y) * 2 + zh2
                    pairs += [(here, there), (there, here)]
    return pairs


def local(positions, features, struct_ids, slots, validity, radial_in, radial_out, mixing, readout):
    atoms = ("x", "zl", "k")
    domains = lax.axis_size(atoms)
    siblings = [(d, d ^ 1) for d in range(domains)]
    crossing = chip_to_chip()
    everyone = ("x", "zl", "k", "y", "zh")
    channels, edges = readout.shape[0], 8 * LANES
    rows = features.shape[0]
    weights = jnp.where(lax.axis_index("k") == 0, radial_out, mixing.T)
    shard = jnp.concatenate([features, weights], axis=1)
    shard_z = lax.ppermute(shard, "zh", [(0, 1), (1, 0)])
    packed = kernel(pack_kernel, [((4, 2 * rows, LANES + channels), BF16)], 4)(shard, shard_z)[0]
    gathered = lax.all_to_all(packed, "y", 0, 0, tiled=True)
    pos_sib = lax.ppermute(positions, atoms, siblings)
    pos_cross = lax.ppermute(positions, everyone, crossing)
    hidden, dhidden, geo = kernel(
        stage_kernel,
        [((channels, edges), BF16), ((channels, edges), BF16), ((4, 8, LANES), F32)],
        16,
        cost=3,
    )(positions, pos_sib, pos_cross, slots, radial_in)
    cross = lax.ppermute(gathered[:, :, :LANES], everyone, crossing)
    swapped = lax.ppermute(gathered, atoms, siblings)
    radial, dradial, mix, mixt = kernel(
        radial_kernel,
        [((channels, edges), F32)] * 2 + [((channels, channels), BF16)] * 2,
        12,
        cost=2,
    )(gathered, swapped, hidden, dhidden)
    message = kernel(
        main_kernel,
        [((32, 8, LANES), F32)],
        20,
        scratch=[
            pltpu.VMEM((channels, 2 * LANES), BF16),
            pltpu.VMEM((channels, LANES), F32),
        ],
        cost=4,
    )(
        gathered,
        swapped,
        cross,
        radial,
        dradial,
        mix,
        mixt,
        geo,
        slots,
        validity,
        struct_ids.reshape(1, LANES),
        readout.reshape(4, LANES),
    )[0]
    got = lax.all_to_all(message, ("x", "y", "k"), 0, 0, tiled=True)
    message = kernel(middle_kernel, [((8, 8, LANES), F32)], 4)(got)[0]
    got = lax.all_to_all(message, ("zl", "zh"), 0, 0, tiled=True)
    return tuple(kernel(final_kernel, [((3, LANES), F32), ((9, STRUCTS), F32)], 4)(got))


def solution(mesh):
    fine = Mesh(mesh.devices.reshape(4, 4, 2, 4, 2), ("x", "zl", "k", "y", "zh"))
    atoms, chans = ("x", "zl", "k"), ("y", "zh")
    placed = (
        P(None, atoms),
        P(chans, atoms),
        P(atoms),
        P(None, atoms),
        P(None, atoms),
        P(),
        P(chans, None),
        P(None, chans),
        P(),
    )
    return jax.shard_map(
        local, mesh=fine, in_specs=placed, out_specs=(P(None, atoms), P()), check_vma=False
    )
```

```python
import jax
import jax.numpy as jnp
from jax import lax
from jax.experimental import pallas as pl
from jax.experimental.pallas import tpu as pltpu
from jax.sharding import Mesh
from jax.sharding import PartitionSpec as P


RIM = 48
LANES = 128
CHUNK = 512
SHARPNESS = 40.0
REACH = 10.0
STRUCTS = 32

VMEM = pl.BlockSpec(memory_space=pltpu.VMEM)
F32 = jnp.float32
BF16 = jnp.bfloat16


def kernel(body, outs, mib, scratch=(), cost=1, space=pltpu.VMEM):
    def call(*args):
        return pl.pallas_call(
            body,
            out_shape=[jax.ShapeDtypeStruct(shape, dtype) for shape, dtype in outs],
            in_specs=[pl.BlockSpec(memory_space=space)] * len(args),
            out_specs=[VMEM] * len(outs),
            scratch_shapes=list(scratch),
            compiler_params=pltpu.CompilerParams(vmem_limit_bytes=mib << 20),
            cost_estimate=pl.CostEstimate(flops=cost * 1_000_000_000, bytes_accessed=100_000, transcendentals=0),
        )(*args)

    return call


def iota(shape, dim):
    return lax.broadcasted_iota(jnp.int32, shape, dim)


def dot(a, b):
    return jnp.dot(a, b, preferred_element_type=F32)


def dot_t(a, b):
    return lax.dot_general(a, b, (((1,), (1,)), ((), ())), preferred_element_type=F32)


def sigmoid(v):
    return 0.5 + 0.5 * jnp.tanh(0.5 * v)


def where_am_i():
    return lax.axis_index("x"), lax.axis_index("zl"), lax.axis_index("k")


def slot_group():
    return lax.axis_index("y") * 2 + lax.axis_index("zh")


def pick_kernel(feat, rout, mixt, shard, sems):
    core = lax.axis_index("k")

    def take(weights):
        moves = (
            pltpu.make_async_copy(weights, shard.at[:, LANES:], sems.at[0]),
            pltpu.make_async_copy(feat, shard.at[:, :LANES], sems.at[1]),
        )
        for move in moves:
            move.start()
        for move in moves:
            move.wait()

    @pl.when(core == 0)
    def _():
        take(rout)

    @pl.when(core != 0)
    def _():
        take(mixt)


def pack_kernel(here_shard, there_shard, out):
    rows = here_shard.shape[0]
    zh = lax.axis_index("zh")
    here, there = pl.multiple_of(zh * rows, rows), pl.multiple_of((1 - zh) * rows, rows)
    for c in range(out.shape[0]):
        out[c, pl.ds(here, rows), :] = here_shard[...]
        out[c, pl.ds(there, rows), :] = there_shard[...]


def halo_of(core, sib, cross, lane):
    low = jnp.where(core == 0, sib, cross)
    high = jnp.where(core == 0, cross, sib)
    return jnp.where(lane < 64, low, high)


def own_rows(ref):
    used = 8
    first = pl.multiple_of(slot_group() * used, used)
    return ref[pl.ds(first, used), :]


def slot_index(slots):
    rows = own_rows(slots)
    return (rows + iota(rows.shape, 1) - RIM) & 255


def stage_kernel(pos, sib, cross, slots, radial_in, hidden, dhidden, geo):
    core = lax.axis_index("k")
    idx = slot_index(slots)
    lane = iota(idx.shape, 1)
    inner = idx & 127
    vecs = []
    for p in range(3):
        own = jnp.broadcast_to(pos[p : p + 1, :], idx.shape)
        ring = halo_of(
            core,
            jnp.broadcast_to(sib[p : p + 1, :], idx.shape),
            jnp.broadcast_to(cross[p : p + 1, :], idx.shape),
            lane,
        )
        far = jnp.where(
            idx < 128,
            jnp.take_along_axis(own, inner, axis=1),
            jnp.take_along_axis(ring, inner, axis=1),
        )
        vecs.append(far - own)
    dist = jnp.sqrt(1.0 + (vecs[0] * vecs[0] + vecs[1] * vecs[1] + vecs[2] * vecs[2]))
    for p in range(3):
        geo[p] = vecs[p]
    geo[3] = dist
    count = radial_in.shape[1]
    centers = iota((count, LANES), 0).astype(F32) * (REACH / count)
    weights = radial_in[...]
    for k in range(8):
        offset = jnp.broadcast_to(dist[k : k + 1, :], (count, LANES)) - centers
        bump = jnp.exp(-SHARPNESS * offset * offset)
        slope = (-2.0 * SHARPNESS * offset * bump).astype(BF16)
        both = jnp.concatenate([bump.astype(BF16), slope], axis=1)
        pre2 = dot(weights, both)
        pre, dpre = pre2[:, :LANES], pre2[:, LANES:]
        sig = sigmoid(pre)
        silu = pre * sig
        at = slice(k * LANES, (k + 1) * LANES)
        hidden[:, at] = silu.astype(BF16)
        dhidden[:, at] = ((sig + silu * (1.0 - sig)) * dpre).astype(BF16)


def radial_kernel(gathered, swapped, hidden, dhidden, radial, dradial, mix, mixt):
    core = lax.axis_index("k")
    channels = mix.shape[0]

    def run(w_rad, w_mixt):
        weights = w_rad[:, :, LANES:].reshape(channels, channels)
        for n in range(hidden.shape[1] // CHUNK):
            at = slice(n * CHUNK, (n + 1) * CHUNK)
            radial[:, at] = dot(weights, hidden[:, at])
            dradial[:, at] = dot(weights, dhidden[:, at])
        turned = w_mixt[:, :, LANES:].reshape(channels, channels)
        mixt[...] = turned
        mix[...] = turned.T

    @pl.when(core == 0)
    def _():
        run(gathered, swapped)

    @pl.when(core != 0)
    def _():
        run(swapped, gathered)


def main_kernel(
    own, sib, cross, radial, dradial, mix, mixt, geo, slots, valid, ids, readout, out, table_f, scale
):
    core = lax.axis_index("k")
    channels = table_f.shape[0]
    lane = iota((channels, LANES), 1)
    own_f = own[:, :, :LANES].reshape(channels, LANES)
    sib_f = sib[:, :, :LANES].reshape(channels, LANES)
    cross_f = cross[...].reshape(channels, LANES)
    table_f[:, :LANES] = own_f
    table_f[:, LANES:] = halo_of(core, sib_f, cross_f, lane)
    turned = jnp.concatenate([readout[...]] * 2, axis=0).T
    for j in range(4):
        scale[j * LANES : (j + 1) * LANES, :] = jnp.broadcast_to(turned[:, j : j + 1], (LANES, LANES))

    idx = slot_index(slots)
    weight = own_rows(valid).astype(F32)
    gdists = []
    onehots = []
    per = CHUNK // LANES

    def forward(n):
        row_of = iota((256, LANES), 0)
        onehot = jnp.concatenate(
            [
                (row_of == jnp.broadcast_to(idx[k : k + 1, :], (256, LANES))).astype(F32).astype(BF16)
                for k in range(n * per, (n + 1) * per)
            ],
            axis=1,
        )
        onehots.append(onehot)
        far = dot(table_f[...], onehot)
        message = (far * radial[:, n * CHUNK : (n + 1) * CHUNK]).astype(BF16)
        return far, dot(mix[...], message)

    def backward(n, far, mixed):
        sig = sigmoid(mixed)
        slope = sig + mixed * sig * (1.0 - sig)
        wide = jnp.concatenate([scale[...]] * per, axis=1)
        gmix = (wide * slope).astype(BF16)
        gmsg = dot(mixt[...], gmix)
        kept = far * dradial[:, n * CHUNK : (n + 1) * CHUNK]
        gdists.append(jnp.sum(gmsg * kept, axis=0, keepdims=True))

    ahead = forward(0)
    for n in range(1024 // CHUNK):
        now = ahead
        if n + 1 < 1024 // CHUNK:
            ahead = forward(n + 1)
        backward(n, *now)
    row8 = iota((8, LANES), 0)
    gdist = jnp.zeros((8, LANES), F32)
    for k in range(8):
        per = CHUNK // LANES
        part = gdists[k // per][:, (k % per) * LANES : (k % per + 1) * LANES]
        gdist = jnp.where(row8 == k, jnp.broadcast_to(part, (8, LANES)), gdist)
    over = gdist * weight / geo[3]
    vecs = [geo[p] for p in range(3)]
    gvec = [over * v for v in vecs]

    def total(v):
        return jnp.broadcast_to(jnp.sum(v, axis=0, keepdims=True), (8, LANES))

    zero = jnp.zeros((8, LANES), F32)
    acc = jnp.zeros((8, 256), F32)
    for k in range(8):
        rows = zero
        for p in range(3):
            rows = jnp.where(row8 == p, jnp.broadcast_to(gvec[p][k : k + 1, :], (8, LANES)), rows)
        per = CHUNK // LANES
        hot = onehots[k // per][:, (k % per) * LANES : (k % per + 1) * LANES]
        rest = rows
        for _ in range(3):
            part = rest.astype(BF16)
            acc = acc + dot_t(part, hot)
            rest = rest - part.astype(F32)
    mine, ring = -acc[:, :LANES], -acc[:, LANES:]
    for p in range(3):
        mine = mine + jnp.where(row8 == p, total(gvec[p]), 0.0)
    pairs = ((0, 0), (0, 1), (0, 2), (1, 1), (1, 2), (2, 2))
    vir = jnp.where(row8 == 6, 1.0, zero)
    for j, (p, q) in enumerate(pairs):
        vir = jnp.where(row8 == j, total(vecs[p] * gvec[q]), vir)
    struct = iota((LANES, LANES), 0) & (STRUCTS - 1)
    member = (struct == jnp.broadcast_to(ids[...], (LANES, LANES))).astype(F32).astype(BF16)
    spread = jnp.zeros((8, LANES), F32)
    rest = vir
    for _ in range(3):
        part = rest.astype(BF16)
        spread = spread + dot_t(part, member)
        rest = rest - part.astype(F32)
    lane8 = iota((8, LANES), 1)
    picked = jnp.where((lane8 >> 5) == (row8 & 3), spread, 0.0)
    first_row = total(jnp.where(row8 < 4, picked, 0.0))
    second_row = total(jnp.where(row8 >= 4, picked, 0.0))
    ring = pltpu.roll(ring, 3, 0)
    result = jnp.where(row8 < 3, mine, jnp.where(row8 < 6, ring, jnp.where(row8 == 6, first_row, second_row)))
    for c in range(out.shape[0]):
        out[c] = result


def middle_kernel(got, out):
    (x, zl, core), nx = where_am_i(), 4
    row8, lane8 = iota((8, LANES), 0), iota((8, LANES), 1)
    edge = jnp.where(core == 0, jnp.where(zl == 3, -1, 0), jnp.where(zl == 0, 1, 0))
    source = x + edge
    inside = jnp.logical_and(source >= 0, source < nx)
    source = jnp.clip(source, 0, nx - 1)
    whole = got[0]
    for i in range(1, got.shape[0]):
        whole = whole + got[i]

    def over_y(xx, kk):
        v = got[xx * 8 + kk]
        for y in range(1, 4):
            v = v + got[xx * 8 + y * 2 + kk]
        return v

    mine = over_y(x, core)
    near = pltpu.roll(over_y(x, 1 - core), 5, 0)
    far = over_y(source, 1 - core)
    far = jnp.where(inside, far, 0.0)
    low = lane8 < 64
    is_first = core == 0
    near_mask = jnp.logical_xor(low, is_first)
    mine = mine + jnp.where(near_mask, near, 0.0)
    far = jnp.where(near_mask, 0.0, far)
    result = jnp.where(row8 < 3, mine, jnp.where(row8 < 6, far, whole))
    for c in range(out.shape[0]):
        out[c] = result


def final_kernel(got, forces, stress):
    _, zl, core = where_am_i()
    whole = got[0]
    for i in range(1, got.shape[0]):
        whole = whole + got[i]
    mine = got[zl * 2] + got[zl * 2 + 1]
    other = (zl + jnp.where(core == 0, 3, 1)) & 3
    ring = got[other * 2] + got[other * 2 + 1]
    forces[...] = mine[:3, :] + ring[3:6, :]
    count = whole[7:8, 64:96] * 0.125
    where_is = {(0, 0): 0, (0, 1): 1, (0, 2): 2, (1, 1): 3, (1, 2): 4, (2, 2): 5}
    for p in range(3):
        for q in range(3):
            j = where_is[(min(p, q), max(p, q))]
            value = whole[6 + j // 4 : 7 + j // 4, (j % 4) * 32 : (j % 4) * 32 + 32]
            stress[3 * p + q : 3 * p + q + 1, :] = -value / count


def chip_to_chip():
    pairs = []
    for x in range(4):
        for zl in range(4):
            for y in range(4):
                for zh in range(2):
                    here = (((x * 4 + zl) * 2 + 1) * 4 + y) * 2 + zh
                    x2, zl2, zh2 = (x + (zl == 3)) % 4, (zl + 1) % 4, zh ^ (zl == 3)
                    there = ((x2 * 4 + zl2) * 2 * 4 + y) * 2 + zh2
                    pairs += [(here, there), (there, here)]
    return pairs


def local(positions, features, struct_ids, slots, validity, radial_in, radial_out, mixing, readout):
    atoms = ("x", "zl", "k")
    domains = lax.axis_size(atoms)
    siblings = [(d, d ^ 1) for d in range(domains)]
    crossing = chip_to_chip()
    everyone = ("x", "zl", "k", "y", "zh")
    channels, edges = readout.shape[0], 8 * LANES
    rows = features.shape[0]
    held = [pltpu.with_memory_space_constraint(a, pltpu.HBM) for a in (features, radial_out, mixing.T)]
    shard = kernel(
        pick_kernel,
        [((rows, LANES + channels), BF16)],
        4,
        scratch=[pltpu.SemaphoreType.DMA((2,))],
        space=pltpu.HBM,
    )(*held)[0]
    shard_z = lax.ppermute(shard, "zh", [(0, 1), (1, 0)])
    packed = kernel(pack_kernel, [((4, 2 * rows, LANES + channels), BF16)], 4)(shard, shard_z)[0]
    gathered = lax.all_to_all(packed, "y", 0, 0, tiled=True)
    pos_sib = lax.ppermute(positions, atoms, siblings)
    pos_cross = lax.ppermute(positions, everyone, crossing)
    hidden, dhidden, geo = kernel(
        stage_kernel,
        [((channels, edges), BF16), ((channels, edges), BF16), ((4, 8, LANES), F32)],
        16,
        cost=3,
    )(positions, pos_sib, pos_cross, slots, radial_in)
    cross = lax.ppermute(gathered[:, :, :LANES], everyone, crossing)
    swapped = lax.ppermute(gathered, atoms, siblings)
    radial, dradial, mix, mixt = kernel(
        radial_kernel,
        [((channels, edges), F32)] * 2 + [((channels, channels), BF16)] * 2,
        12,
        cost=2,
    )(gathered, swapped, hidden, dhidden)
    message = kernel(
        main_kernel,
        [((32, 8, LANES), F32)],
        32,
        scratch=[
            pltpu.VMEM((channels, 2 * LANES), BF16),
            pltpu.VMEM((channels, LANES), F32),
        ],
        cost=4,
    )(
        gathered,
        swapped,
        cross,
        radial,
        dradial,
        mix,
        mixt,
        geo,
        slots,
        validity,
        struct_ids.reshape(1, LANES),
        readout.reshape(4, LANES),
    )[0]
    got = lax.all_to_all(message, ("x", "y", "k"), 0, 0, tiled=True)
    message = kernel(middle_kernel, [((8, 8, LANES), F32)], 4)(got)[0]
    got = lax.all_to_all(message, ("zl", "zh"), 0, 0, tiled=True)
    return tuple(kernel(final_kernel, [((3, LANES), F32), ((9, STRUCTS), F32)], 4)(got))


def solution(mesh):
    fine = Mesh(mesh.devices.reshape(4, 4, 2, 4, 2), ("x", "zl", "k", "y", "zh"))
    atoms, chans = ("x", "zl", "k"), ("y", "zh")
    placed = (
        P(None, atoms),
        P(chans, atoms),
        P(atoms),
        P(None, atoms),
        P(None, atoms),
        P(),
        P(chans, None),
        P(None, chans),
        P(),
    )
    return jax.shard_map(
        local, mesh=fine, in_specs=placed, out_specs=(P(None, atoms), P()), check_vma=False
    )
```

```python
import jax
import jax.numpy as jnp
from jax import lax
from jax.experimental import pallas as pl
from jax.experimental.pallas import tpu as pltpu
from jax.sharding import Mesh
from jax.sharding import PartitionSpec as P


RIM = 48
LANES = 128
CHUNK = 512
SHARPNESS = 40.0
REACH = 10.0
STRUCTS = 32

VMEM = pl.BlockSpec(memory_space=pltpu.VMEM)
F32 = jnp.float32
BF16 = jnp.bfloat16


def kernel(body, outs, mib, scratch=(), cost=1, space=pltpu.VMEM):
    def call(*args):
        return pl.pallas_call(
            body,
            out_shape=[jax.ShapeDtypeStruct(shape, dtype) for shape, dtype in outs],
            in_specs=[pl.BlockSpec(memory_space=space)] * len(args),
            out_specs=[VMEM] * len(outs),
            scratch_shapes=list(scratch),
            compiler_params=pltpu.CompilerParams(vmem_limit_bytes=mib << 20),
            cost_estimate=pl.CostEstimate(flops=cost * 1_000_000_000, bytes_accessed=100_000, transcendentals=0),
        )(*args)

    return call


def iota(shape, dim):
    return lax.broadcasted_iota(jnp.int32, shape, dim)


def dot(a, b):
    return jnp.dot(a, b, preferred_element_type=F32)


def dot_t(a, b):
    return lax.dot_general(a, b, (((1,), (1,)), ((), ())), preferred_element_type=F32)


def exact_dot_t(a, b):
    parts, rest = [], a
    for _ in range(3):
        parts.append(rest.astype(BF16).astype(F32))
        rest = rest - parts[-1]
    sums = dot_t(jnp.concatenate(parts, axis=0).astype(BF16), b)
    return sums[0:8] + sums[8:16] + sums[16:24]


def sigmoid(v):
    return 0.5 + 0.5 * jnp.tanh(0.5 * v)


def where_am_i():
    return lax.axis_index("x"), lax.axis_index("zl"), lax.axis_index("k")


def slot_group():
    return lax.axis_index("y") * 2 + lax.axis_index("zh")


def pick_kernel(feat, rout, mixt, shard, sems):
    core = lax.axis_index("k")

    def take(weights):
        moves = (
            pltpu.make_async_copy(weights, shard.at[:, LANES:], sems.at[0]),
            pltpu.make_async_copy(feat, shard.at[:, :LANES], sems.at[1]),
        )
        for move in moves:
            move.start()
        for move in moves:
            move.wait()

    @pl.when(core == 0)
    def _():
        take(rout)

    @pl.when(core != 0)
    def _():
        take(mixt)


def pack_kernel(here_shard, there_shard, out):
    rows = here_shard.shape[0]
    zh = lax.axis_index("zh")
    here, there = pl.multiple_of(zh * rows, rows), pl.multiple_of((1 - zh) * rows, rows)
    for c in range(out.shape[0]):
        out[c, pl.ds(here, rows), :] = here_shard[...]
        out[c, pl.ds(there, rows), :] = there_shard[...]


def halo_of(core, sib, cross, lane):
    low = jnp.where(core == 0, sib, cross)
    high = jnp.where(core == 0, cross, sib)
    return jnp.where(lane < 64, low, high)


def own_rows(ref):
    used = 8
    first = pl.multiple_of(slot_group() * used, used)
    return ref[pl.ds(first, used), :]


def slot_index(slots):
    rows = own_rows(slots)
    return (rows + iota(rows.shape, 1) - RIM) & 255


def stage_kernel(pos, sib, cross, slots, radial_in, hidden, dhidden, geo):
    core = lax.axis_index("k")
    idx = slot_index(slots)
    lane = iota(idx.shape, 1)
    inner = idx & 127
    vecs = []
    for p in range(3):
        own = jnp.broadcast_to(pos[p : p + 1, :], idx.shape)
        ring = halo_of(
            core,
            jnp.broadcast_to(sib[p : p + 1, :], idx.shape),
            jnp.broadcast_to(cross[p : p + 1, :], idx.shape),
            lane,
        )
        far = jnp.where(
            idx < 128,
            jnp.take_along_axis(own, inner, axis=1),
            jnp.take_along_axis(ring, inner, axis=1),
        )
        vecs.append(far - own)
    dist = jnp.sqrt(1.0 + (vecs[0] * vecs[0] + vecs[1] * vecs[1] + vecs[2] * vecs[2]))
    for p in range(3):
        geo[p] = vecs[p]
    geo[3] = dist
    count = radial_in.shape[1]
    centers = iota((count, LANES), 0).astype(F32) * (REACH / count)
    weights = radial_in[...]
    for k in range(8):
        offset = jnp.broadcast_to(dist[k : k + 1, :], (count, LANES)) - centers
        bump = jnp.exp(-SHARPNESS * offset * offset)
        slope = (-2.0 * SHARPNESS * offset * bump).astype(BF16)
        both = jnp.concatenate([bump.astype(BF16), slope], axis=1)
        pre2 = dot(weights, both)
        pre, dpre = pre2[:, :LANES], pre2[:, LANES:]
        sig = sigmoid(pre)
        silu = pre * sig
        at = slice(k * LANES, (k + 1) * LANES)
        hidden[:, at] = silu.astype(BF16)
        dhidden[:, at] = ((sig + silu * (1.0 - sig)) * dpre).astype(BF16)


def radial_kernel(gathered, swapped, hidden, dhidden, radial, dradial, mix, mixt):
    core = lax.axis_index("k")
    channels = mix.shape[0]

    def run(w_rad, w_mixt):
        weights = w_rad[:, :, LANES:].reshape(channels, channels)
        for n in range(hidden.shape[1] // CHUNK):
            at = slice(n * CHUNK, (n + 1) * CHUNK)
            radial[:, at] = dot(weights, hidden[:, at])
            dradial[:, at] = dot(weights, dhidden[:, at])
        turned = w_mixt[:, :, LANES:].reshape(channels, channels)
        mixt[...] = turned
        mix[...] = turned.T

    @pl.when(core == 0)
    def _():
        run(gathered, swapped)

    @pl.when(core != 0)
    def _():
        run(swapped, gathered)


def main_kernel(
    own, sib, cross, radial, dradial, mix, mixt, geo, slots, valid, ids, readout, out, table_f, scale
):
    core = lax.axis_index("k")
    channels = table_f.shape[0]
    lane = iota((channels, LANES), 1)
    own_f = own[:, :, :LANES].reshape(channels, LANES)
    sib_f = sib[:, :, :LANES].reshape(channels, LANES)
    cross_f = cross[...].reshape(channels, LANES)
    table_f[:, :LANES] = own_f
    table_f[:, LANES:] = halo_of(core, sib_f, cross_f, lane)
    turned = jnp.concatenate([readout[...]] * 2, axis=0).T
    for j in range(4):
        scale[j * LANES : (j + 1) * LANES, :] = jnp.broadcast_to(turned[:, j : j + 1], (LANES, LANES))

    idx = slot_index(slots)
    weight = own_rows(valid).astype(F32)
    gdists = []
    onehots = []
    per = CHUNK // LANES

    def forward(n):
        row_of = iota((256, LANES), 0)
        onehot = jnp.concatenate(
            [
                (row_of == jnp.broadcast_to(idx[k : k + 1, :], (256, LANES))).astype(F32).astype(BF16)
                for k in range(n * per, (n + 1) * per)
            ],
            axis=1,
        )
        onehots.append(onehot)
        far = dot(table_f[...], onehot)
        message = (far * radial[:, n * CHUNK : (n + 1) * CHUNK]).astype(BF16)
        return far, dot(mix[...], message)

    def backward(n, far, mixed):
        sig = sigmoid(mixed)
        slope = sig + mixed * sig * (1.0 - sig)
        wide = jnp.concatenate([scale[...]] * per, axis=1)
        gmix = (wide * slope).astype(BF16)
        gmsg = dot(mixt[...], gmix)
        kept = far * dradial[:, n * CHUNK : (n + 1) * CHUNK]
        gdists.append(jnp.sum(gmsg * kept, axis=0, keepdims=True))

    ahead = forward(0)
    for n in range(1024 // CHUNK):
        now = ahead
        if n + 1 < 1024 // CHUNK:
            ahead = forward(n + 1)
        backward(n, *now)
    row8 = iota((8, LANES), 0)
    gdist = jnp.zeros((8, LANES), F32)
    for k in range(8):
        per = CHUNK // LANES
        part = gdists[k // per][:, (k % per) * LANES : (k % per + 1) * LANES]
        gdist = jnp.where(row8 == k, jnp.broadcast_to(part, (8, LANES)), gdist)
    over = gdist * weight / geo[3]
    vecs = [geo[p] for p in range(3)]
    gvec = [over * v for v in vecs]

    def total(v):
        return jnp.broadcast_to(jnp.sum(v, axis=0, keepdims=True), (8, LANES))

    zero = jnp.zeros((8, LANES), F32)
    blocks = []
    for k in range(8):
        rows = zero
        for p in range(3):
            rows = jnp.where(row8 == p, jnp.broadcast_to(gvec[p][k : k + 1, :], (8, LANES)), rows)
        blocks.append(rows)
    acc = jnp.zeros((8, 256), F32)
    for n, hot in enumerate(onehots):
        acc = acc + exact_dot_t(jnp.concatenate(blocks[n * per : (n + 1) * per], axis=1), hot)
    mine, ring = -acc[:, :LANES], -acc[:, LANES:]
    for p in range(3):
        mine = mine + jnp.where(row8 == p, total(gvec[p]), 0.0)
    pairs = ((0, 0), (0, 1), (0, 2), (1, 1), (1, 2), (2, 2))
    vir = jnp.where(row8 == 6, 1.0, zero)
    for j, (p, q) in enumerate(pairs):
        vir = jnp.where(row8 == j, total(vecs[p] * gvec[q]), vir)
    struct = iota((LANES, LANES), 0) & (STRUCTS - 1)
    member = (struct == jnp.broadcast_to(ids[...], (LANES, LANES))).astype(F32).astype(BF16)
    spread = exact_dot_t(vir, member)
    lane8 = iota((8, LANES), 1)
    picked = jnp.where((lane8 >> 5) == (row8 & 3), spread, 0.0)
    first_row = total(jnp.where(row8 < 4, picked, 0.0))
    second_row = total(jnp.where(row8 >= 4, picked, 0.0))
    ring = pltpu.roll(ring, 3, 0)
    result = jnp.where(row8 < 3, mine, jnp.where(row8 < 6, ring, jnp.where(row8 == 6, first_row, second_row)))
    for c in range(out.shape[0]):
        out[c] = result


def middle_kernel(got, out):
    (x, zl, core), nx = where_am_i(), 4
    row8, lane8 = iota((8, LANES), 0), iota((8, LANES), 1)
    edge = jnp.where(core == 0, jnp.where(zl == 3, -1, 0), jnp.where(zl == 0, 1, 0))
    source = x + edge
    inside = jnp.logical_and(source >= 0, source < nx)
    source = jnp.clip(source, 0, nx - 1)
    whole = got[0]
    for i in range(1, got.shape[0]):
        whole = whole + got[i]

    def over_y(xx, kk):
        v = got[xx * 8 + kk]
        for y in range(1, 4):
            v = v + got[xx * 8 + y * 2 + kk]
        return v

    mine = over_y(x, core)
    near = pltpu.roll(over_y(x, 1 - core), 5, 0)
    far = over_y(source, 1 - core)
    far = jnp.where(inside, far, 0.0)
    low = lane8 < 64
    is_first = core == 0
    near_mask = jnp.logical_xor(low, is_first)
    mine = mine + jnp.where(near_mask, near, 0.0)
    far = jnp.where(near_mask, 0.0, far)
    result = jnp.where(row8 < 3, mine, jnp.where(row8 < 6, far, whole))
    for c in range(out.shape[0]):
        out[c] = result


def final_kernel(got, forces, stress):
    _, zl, core = where_am_i()
    whole = got[0]
    for i in range(1, got.shape[0]):
        whole = whole + got[i]
    mine = got[zl * 2] + got[zl * 2 + 1]
    other = (zl + jnp.where(core == 0, 3, 1)) & 3
    ring = got[other * 2] + got[other * 2 + 1]
    forces[...] = mine[:3, :] + ring[3:6, :]
    count = whole[7:8, 64:96] * 0.125
    where_is = {(0, 0): 0, (0, 1): 1, (0, 2): 2, (1, 1): 3, (1, 2): 4, (2, 2): 5}
    for p in range(3):
        for q in range(3):
            j = where_is[(min(p, q), max(p, q))]
            value = whole[6 + j // 4 : 7 + j // 4, (j % 4) * 32 : (j % 4) * 32 + 32]
            stress[3 * p + q : 3 * p + q + 1, :] = -value / count


def chip_to_chip():
    pairs = []
    for x in range(4):
        for zl in range(4):
            for y in range(4):
                for zh in range(2):
                    here = (((x * 4 + zl) * 2 + 1) * 4 + y) * 2 + zh
                    x2, zl2, zh2 = (x + (zl == 3)) % 4, (zl + 1) % 4, zh ^ (zl == 3)
                    there = ((x2 * 4 + zl2) * 2 * 4 + y) * 2 + zh2
                    pairs += [(here, there), (there, here)]
    return pairs


def local(positions, features, struct_ids, slots, validity, radial_in, radial_out, mixing, readout):
    atoms = ("x", "zl", "k")
    domains = lax.axis_size(atoms)
    siblings = [(d, d ^ 1) for d in range(domains)]
    crossing = chip_to_chip()
    everyone = ("x", "zl", "k", "y", "zh")
    channels, edges = readout.shape[0], 8 * LANES
    rows = features.shape[0]
    held = [pltpu.with_memory_space_constraint(a, pltpu.HBM) for a in (features, radial_out, mixing.T)]
    shard = kernel(
        pick_kernel,
        [((rows, LANES + channels), BF16)],
        4,
        scratch=[pltpu.SemaphoreType.DMA((2,))],
        space=pltpu.HBM,
    )(*held)[0]
    shard_z = lax.ppermute(shard, "zh", [(0, 1), (1, 0)])
    packed = kernel(pack_kernel, [((4, 2 * rows, LANES + channels), BF16)], 4)(shard, shard_z)[0]
    gathered = lax.all_to_all(packed, "y", 0, 0, tiled=True)
    pos_sib = lax.ppermute(positions, atoms, siblings)
    pos_cross = lax.ppermute(positions, everyone, crossing)
    hidden, dhidden, geo = kernel(
        stage_kernel,
        [((channels, edges), BF16), ((channels, edges), BF16), ((4, 8, LANES), F32)],
        16,
        cost=3,
    )(positions, pos_sib, pos_cross, slots, radial_in)
    cross = lax.ppermute(gathered[:, :, :LANES], everyone, crossing)
    swapped = lax.ppermute(gathered, atoms, siblings)
    radial, dradial, mix, mixt = kernel(
        radial_kernel,
        [((channels, edges), F32)] * 2 + [((channels, channels), BF16)] * 2,
        12,
        cost=2,
    )(gathered, swapped, hidden, dhidden)
    message = kernel(
        main_kernel,
        [((32, 8, LANES), F32)],
        32,
        scratch=[
            pltpu.VMEM((channels, 2 * LANES), BF16),
            pltpu.VMEM((channels, LANES), F32),
        ],
        cost=4,
    )(
        gathered,
        swapped,
        cross,
        radial,
        dradial,
        mix,
        mixt,
        geo,
        slots,
        validity,
        struct_ids.reshape(1, LANES),
        readout.reshape(4, LANES),
    )[0]
    got = lax.all_to_all(message, ("x", "y", "k"), 0, 0, tiled=True)
    message = kernel(middle_kernel, [((8, 8, LANES), F32)], 4)(got)[0]
    got = lax.all_to_all(message, ("zl", "zh"), 0, 0, tiled=True)
    return tuple(kernel(final_kernel, [((3, LANES), F32), ((9, STRUCTS), F32)], 4)(got))


def solution(mesh):
    fine = Mesh(mesh.devices.reshape(4, 4, 2, 4, 2), ("x", "zl", "k", "y", "zh"))
    atoms, chans = ("x", "zl", "k"), ("y", "zh")
    placed = (
        P(None, atoms),
        P(chans, atoms),
        P(atoms),
        P(None, atoms),
        P(None, atoms),
        P(),
        P(chans, None),
        P(None, chans),
        P(),
    )
    return jax.shard_map(
        local, mesh=fine, in_specs=placed, out_specs=(P(None, atoms), P()), check_vma=False
    )
```

```python
import jax
import jax.numpy as jnp
from jax import lax
from jax.experimental import pallas as pl
from jax.experimental.pallas import tpu as pltpu
from jax.sharding import Mesh
from jax.sharding import PartitionSpec as P


RIM = 48
LANES = 128
CHUNK = 512
SHARPNESS = 40.0
REACH = 10.0
STRUCTS = 32

VMEM = pl.BlockSpec(memory_space=pltpu.VMEM)
F32 = jnp.float32
BF16 = jnp.bfloat16


def kernel(body, outs, mib, scratch=(), cost=1, space=pltpu.VMEM):
    def call(*args):
        return pl.pallas_call(
            body,
            out_shape=[jax.ShapeDtypeStruct(shape, dtype) for shape, dtype in outs],
            in_specs=[pl.BlockSpec(memory_space=space)] * len(args),
            out_specs=[VMEM] * len(outs),
            scratch_shapes=list(scratch),
            compiler_params=pltpu.CompilerParams(vmem_limit_bytes=mib << 20),
            cost_estimate=pl.CostEstimate(flops=cost * 1_000_000_000, bytes_accessed=100_000, transcendentals=0),
        )(*args)

    return call


def iota(shape, dim):
    return lax.broadcasted_iota(jnp.int32, shape, dim)


def dot(a, b):
    return jnp.dot(a, b, preferred_element_type=F32)


def dot_t(a, b):
    return lax.dot_general(a, b, (((1,), (1,)), ((), ())), preferred_element_type=F32)


def exact_dot_t(a, b):
    parts, rest = [], a
    for _ in range(3):
        parts.append(rest.astype(BF16).astype(F32))
        rest = rest - parts[-1]
    sums = dot_t(jnp.concatenate(parts, axis=0).astype(BF16), b)
    return sums[0:8] + sums[8:16] + sums[16:24]


def where_am_i():
    return lax.axis_index("x"), lax.axis_index("zl"), lax.axis_index("k")


def slot_group():
    return lax.axis_index("y") * 2 + lax.axis_index("zh")


def pick_kernel(feat, rout, mixt, shard, sems):
    core = lax.axis_index("k")

    def take(weights):
        moves = (
            pltpu.make_async_copy(weights, shard.at[:, LANES:], sems.at[0]),
            pltpu.make_async_copy(feat, shard.at[:, :LANES], sems.at[1]),
        )
        for move in moves:
            move.start()
        for move in moves:
            move.wait()

    @pl.when(core == 0)
    def _():
        take(rout)

    @pl.when(core != 0)
    def _():
        take(mixt)


def pack_kernel(here_shard, there_shard, out):
    rows = here_shard.shape[0]
    zh = lax.axis_index("zh")
    here, there = pl.multiple_of(zh * rows, rows), pl.multiple_of((1 - zh) * rows, rows)
    for c in range(out.shape[0]):
        out[c, pl.ds(here, rows), :] = here_shard[...]
        out[c, pl.ds(there, rows), :] = there_shard[...]


def halo_of(core, sib, cross, lane):
    low = jnp.where(core == 0, sib, cross)
    high = jnp.where(core == 0, cross, sib)
    return jnp.where(lane < 64, low, high)


def own_rows(ref):
    used = 8
    first = pl.multiple_of(slot_group() * used, used)
    return ref[pl.ds(first, used), :]


def slot_index(slots):
    rows = own_rows(slots)
    return (rows + iota(rows.shape, 1) - RIM) & 255


def stage_kernel(pos, sib, cross, slots, radial_in, hidden, dhidden, geo):
    core = lax.axis_index("k")
    idx = slot_index(slots)
    lane = iota(idx.shape, 1)
    inner = idx & 127
    vecs = []
    for p in range(3):
        own = jnp.broadcast_to(pos[p : p + 1, :], idx.shape)
        ring = halo_of(
            core,
            jnp.broadcast_to(sib[p : p + 1, :], idx.shape),
            jnp.broadcast_to(cross[p : p + 1, :], idx.shape),
            lane,
        )
        far = jnp.where(
            idx < 128,
            jnp.take_along_axis(own, inner, axis=1),
            jnp.take_along_axis(ring, inner, axis=1),
        )
        vecs.append(far - own)
    dist = jnp.sqrt(1.0 + (vecs[0] * vecs[0] + vecs[1] * vecs[1] + vecs[2] * vecs[2]))
    for p in range(3):
        geo[p] = vecs[p]
    geo[3] = dist
    count = radial_in.shape[1]
    centers = iota((count, LANES), 0).astype(F32) * (REACH / count)
    weights = (radial_in[...].astype(F32) * 0.5).astype(BF16)
    for k in range(8):
        offset = jnp.broadcast_to(dist[k : k + 1, :], (count, LANES)) - centers
        bump = jnp.exp(-SHARPNESS * offset * offset)
        slope = (-2.0 * SHARPNESS * offset * bump).astype(BF16)
        both = jnp.concatenate([bump.astype(BF16), slope], axis=1)
        pre2 = dot(weights, both)
        half, dhalf = pre2[:, :LANES], pre2[:, LANES:]
        turn = jnp.tanh(half)
        rise = 1.0 + turn
        at = slice(k * LANES, (k + 1) * LANES)
        hidden[:, at] = (half * rise).astype(BF16)
        dhidden[:, at] = (rise * (1.0 + half * (1.0 - turn)) * dhalf).astype(BF16)


def radial_kernel(gathered, swapped, hidden, dhidden, radial, dradial, mix, mixt):
    core = lax.axis_index("k")
    channels = mix.shape[0]

    def run(w_rad, w_mixt):
        weights = w_rad[:, :, LANES:].reshape(channels, channels)
        for n in range(hidden.shape[1] // CHUNK):
            at = slice(n * CHUNK, (n + 1) * CHUNK)
            radial[:, at] = dot(weights, hidden[:, at])
            dradial[:, at] = dot(weights, dhidden[:, at])
        turned = w_mixt[:, :, LANES:].reshape(channels, channels)
        mixt[...] = turned
        mix[...] = (turned.astype(F32) * 0.5).astype(BF16).T

    @pl.when(core == 0)
    def _():
        run(gathered, swapped)

    @pl.when(core != 0)
    def _():
        run(swapped, gathered)


def main_kernel(
    own, sib, cross, radial, dradial, mix, mixt, geo, slots, valid, ids, readout, out, table_f, scale
):
    core = lax.axis_index("k")
    channels = table_f.shape[0]
    lane = iota((channels, LANES), 1)
    own_f = own[:, :, :LANES].reshape(channels, LANES)
    sib_f = sib[:, :, :LANES].reshape(channels, LANES)
    cross_f = cross[...].reshape(channels, LANES)
    table_f[:, :LANES] = own_f
    table_f[:, LANES:] = halo_of(core, sib_f, cross_f, lane)
    turned = jnp.concatenate([readout[...]] * 2, axis=0).T
    for j in range(4):
        scale[j * LANES : (j + 1) * LANES, :] = jnp.broadcast_to(0.5 * turned[:, j : j + 1], (LANES, LANES))

    idx = slot_index(slots)
    weight = own_rows(valid).astype(F32)
    gdists = []
    onehots = []
    per = CHUNK // LANES

    def forward(n):
        row_of = iota((256, LANES), 0)
        onehot = jnp.concatenate(
            [
                (row_of == jnp.broadcast_to(idx[k : k + 1, :], (256, LANES))).astype(F32).astype(BF16)
                for k in range(n * per, (n + 1) * per)
            ],
            axis=1,
        )
        onehots.append(onehot)
        far = dot(table_f[...], onehot)
        message = (far * radial[:, n * CHUNK : (n + 1) * CHUNK]).astype(BF16)
        return far, dot(mix[...], message)

    def backward(n, far, mixed):
        turn = jnp.tanh(mixed)
        slope = (1.0 + turn) * (1.0 + mixed * (1.0 - turn))
        wide = jnp.concatenate([scale[...]] * per, axis=1)
        gmix = (wide * slope).astype(BF16)
        gmsg = dot(mixt[...], gmix)
        kept = far * dradial[:, n * CHUNK : (n + 1) * CHUNK]
        gdists.append(jnp.sum(gmsg * kept, axis=0, keepdims=True))

    ahead = forward(0)
    for n in range(1024 // CHUNK):
        now = ahead
        if n + 1 < 1024 // CHUNK:
            ahead = forward(n + 1)
        backward(n, *now)
    row8 = iota((8, LANES), 0)
    gdist = jnp.zeros((8, LANES), F32)
    for k in range(8):
        per = CHUNK // LANES
        part = gdists[k // per][:, (k % per) * LANES : (k % per + 1) * LANES]
        gdist = jnp.where(row8 == k, jnp.broadcast_to(part, (8, LANES)), gdist)
    over = gdist * weight / geo[3]
    vecs = [geo[p] for p in range(3)]
    gvec = [over * v for v in vecs]

    def total(v):
        return jnp.broadcast_to(jnp.sum(v, axis=0, keepdims=True), (8, LANES))

    zero = jnp.zeros((8, LANES), F32)
    blocks = []
    for k in range(8):
        rows = zero
        for p in range(3):
            rows = jnp.where(row8 == p, jnp.broadcast_to(gvec[p][k : k + 1, :], (8, LANES)), rows)
        blocks.append(rows)
    acc = jnp.zeros((8, 256), F32)
    for n, hot in enumerate(onehots):
        acc = acc + exact_dot_t(jnp.concatenate(blocks[n * per : (n + 1) * per], axis=1), hot)
    mine, ring = -acc[:, :LANES], -acc[:, LANES:]
    for p in range(3):
        mine = mine + jnp.where(row8 == p, total(gvec[p]), 0.0)
    pairs = ((0, 0), (0, 1), (0, 2), (1, 1), (1, 2), (2, 2))
    vir = jnp.where(row8 == 6, 1.0, zero)
    for j, (p, q) in enumerate(pairs):
        vir = jnp.where(row8 == j, total(vecs[p] * gvec[q]), vir)
    struct = iota((LANES, LANES), 0) & (STRUCTS - 1)
    member = (struct == jnp.broadcast_to(ids[...], (LANES, LANES))).astype(F32).astype(BF16)
    spread = exact_dot_t(vir, member)
    lane8 = iota((8, LANES), 1)
    picked = jnp.where((lane8 >> 5) == (row8 & 3), spread, 0.0)
    first_row = total(jnp.where(row8 < 4, picked, 0.0))
    second_row = total(jnp.where(row8 >= 4, picked, 0.0))
    ring = pltpu.roll(ring, 3, 0)
    result = jnp.where(row8 < 3, mine, jnp.where(row8 < 6, ring, jnp.where(row8 == 6, first_row, second_row)))
    for c in range(out.shape[0]):
        out[c] = result


def middle_kernel(got, out):
    (x, zl, core), nx = where_am_i(), 4
    row8, lane8 = iota((8, LANES), 0), iota((8, LANES), 1)
    edge = jnp.where(core == 0, jnp.where(zl == 3, -1, 0), jnp.where(zl == 0, 1, 0))
    source = x + edge
    inside = jnp.logical_and(source >= 0, source < nx)
    source = jnp.clip(source, 0, nx - 1)
    whole = got[0]
    for i in range(1, got.shape[0]):
        whole = whole + got[i]

    def over_y(xx, kk):
        v = got[xx * 8 + kk]
        for y in range(1, 4):
            v = v + got[xx * 8 + y * 2 + kk]
        return v

    mine = over_y(x, core)
    near = pltpu.roll(over_y(x, 1 - core), 5, 0)
    far = over_y(source, 1 - core)
    far = jnp.where(inside, far, 0.0)
    low = lane8 < 64
    is_first = core == 0
    near_mask = jnp.logical_xor(low, is_first)
    mine = mine + jnp.where(near_mask, near, 0.0)
    far = jnp.where(near_mask, 0.0, far)
    result = jnp.where(row8 < 3, mine, jnp.where(row8 < 6, far, whole))
    for c in range(out.shape[0]):
        out[c] = result


def final_kernel(got, forces, stress):
    _, zl, core = where_am_i()
    whole = got[0]
    for i in range(1, got.shape[0]):
        whole = whole + got[i]
    mine = got[zl * 2] + got[zl * 2 + 1]
    other = (zl + jnp.where(core == 0, 3, 1)) & 3
    ring = got[other * 2] + got[other * 2 + 1]
    forces[...] = mine[:3, :] + ring[3:6, :]
    count = whole[7:8, 64:96] * 0.125
    where_is = {(0, 0): 0, (0, 1): 1, (0, 2): 2, (1, 1): 3, (1, 2): 4, (2, 2): 5}
    for p in range(3):
        for q in range(3):
            j = where_is[(min(p, q), max(p, q))]
            value = whole[6 + j // 4 : 7 + j // 4, (j % 4) * 32 : (j % 4) * 32 + 32]
            stress[3 * p + q : 3 * p + q + 1, :] = -value / count


def chip_to_chip():
    pairs = []
    for x in range(4):
        for zl in range(4):
            for y in range(4):
                for zh in range(2):
                    here = (((x * 4 + zl) * 2 + 1) * 4 + y) * 2 + zh
                    x2, zl2, zh2 = (x + (zl == 3)) % 4, (zl + 1) % 4, zh ^ (zl == 3)
                    there = ((x2 * 4 + zl2) * 2 * 4 + y) * 2 + zh2
                    pairs += [(here, there), (there, here)]
    return pairs


def local(positions, features, struct_ids, slots, validity, radial_in, radial_out, mixing, readout):
    atoms = ("x", "zl", "k")
    domains = lax.axis_size(atoms)
    siblings = [(d, d ^ 1) for d in range(domains)]
    crossing = chip_to_chip()
    everyone = ("x", "zl", "k", "y", "zh")
    channels, edges = readout.shape[0], 8 * LANES
    rows = features.shape[0]
    held = [pltpu.with_memory_space_constraint(a, pltpu.HBM) for a in (features, radial_out, mixing.T)]
    shard = kernel(
        pick_kernel,
        [((rows, LANES + channels), BF16)],
        4,
        scratch=[pltpu.SemaphoreType.DMA((2,))],
        space=pltpu.HBM,
    )(*held)[0]
    shard_z = lax.ppermute(shard, "zh", [(0, 1), (1, 0)])
    packed = kernel(pack_kernel, [((4, 2 * rows, LANES + channels), BF16)], 4)(shard, shard_z)[0]
    gathered = lax.all_to_all(packed, "y", 0, 0, tiled=True)
    pos_sib = lax.ppermute(positions, atoms, siblings)
    pos_cross = lax.ppermute(positions, everyone, crossing)
    hidden, dhidden, geo = kernel(
        stage_kernel,
        [((channels, edges), BF16), ((channels, edges), BF16), ((4, 8, LANES), F32)],
        16,
        cost=3,
    )(positions, pos_sib, pos_cross, slots, radial_in)
    cross = lax.ppermute(gathered[:, :, :LANES], everyone, crossing)
    swapped = lax.ppermute(gathered, atoms, siblings)
    radial, dradial, mix, mixt = kernel(
        radial_kernel,
        [((channels, edges), F32)] * 2 + [((channels, channels), BF16)] * 2,
        12,
        cost=2,
    )(gathered, swapped, hidden, dhidden)
    message = kernel(
        main_kernel,
        [((32, 8, LANES), F32)],
        32,
        scratch=[
            pltpu.VMEM((channels, 2 * LANES), BF16),
            pltpu.VMEM((channels, LANES), F32),
        ],
        cost=4,
    )(
        gathered,
        swapped,
        cross,
        radial,
        dradial,
        mix,
        mixt,
        geo,
        slots,
        validity,
        struct_ids.reshape(1, LANES),
        readout.reshape(4, LANES),
    )[0]
    got = lax.all_to_all(message, ("x", "y", "k"), 0, 0, tiled=True)
    message = kernel(middle_kernel, [((8, 8, LANES), F32)], 4)(got)[0]
    got = lax.all_to_all(message, ("zl", "zh"), 0, 0, tiled=True)
    return tuple(kernel(final_kernel, [((3, LANES), F32), ((9, STRUCTS), F32)], 4)(got))


def solution(mesh):
    fine = Mesh(mesh.devices.reshape(4, 4, 2, 4, 2), ("x", "zl", "k", "y", "zh"))
    atoms, chans = ("x", "zl", "k"), ("y", "zh")
    placed = (
        P(None, atoms),
        P(chans, atoms),
        P(atoms),
        P(None, atoms),
        P(None, atoms),
        P(),
        P(chans, None),
        P(None, chans),
        P(),
    )
    return jax.shard_map(
        local, mesh=fine, in_specs=placed, out_specs=(P(None, atoms), P()), check_vma=False
    )
```
